8 devices in a mesh: batch: 1 (over z), z: 2 (over y), y: 2 (over x), x: 2 (over core).
Axes of the slice: x: 2, y: 2, z: 1, core: 2. Of those that a mesh axis runs over, the one named last changes fastest.
Arguments:
- u_init: float32 [64, 64, 64], P(('batch', 'x'), 'y', 'z')
- source: float32 [64, 64, 64], P(('batch', 'x'), 'y', 'z')
- kappa_cell: float32 [64, 64, 64], P(('batch', 'x'), 'y', 'z')
- stencil_w: float32 [26], replicated
- omega_relax: float32 [32], replicated
Outputs:
- output 1: float32 [64, 64, 64], P(('batch', 'x'), 'y', 'z')
- output 2: float32 [32], P('batch')
All inputs are finite; a program needn't handle non-finite values.
Results may differ from the reference program's by a relative error of at most 0.001.
Values are sent between devices in bfloat16 or wider.
A program may use at most 1 GiB of HBM per device.

```python
import jax
import jax.numpy as jnp
from jax import lax

GRID_X = 64
GRID_Y = 64
GRID_Z = 64
SWEEPS = 32
CELLS = GRID_X * GRID_Y * GRID_Z


def stencil_offsets():
    return [(off_a, off_b, off_c) for off_a in (-1, 0, 1) for off_b in (-1, 0, 1) for off_c in (-1, 0, 1) if (off_a, off_b, off_c) != (0, 0, 0)]


def neighbour(values, offset):
    return jnp.roll(values, (-offset[0], -offset[1], -offset[2]), axis=(0, 1, 2))


def setup_inputs(seed: int = 0, part: int = 0) -> dict:
    base_key = jax.random.key(seed)
    shared_key, part_root = jax.random.split(base_key)
    part_key = jax.random.fold_in(part_root, part)
    key_u, key_f, key_k = jax.random.split(part_key, 3)
    key_w, key_o = jax.random.split(shared_key)
    grid_shape = (GRID_X, GRID_Y, GRID_Z)
    u_init = jax.random.normal(key_u, grid_shape, jnp.float32)
    source = jax.random.normal(key_f, grid_shape, jnp.float32)
    kappa_cell = jnp.exp(jax.random.uniform(key_k, grid_shape, jnp.float32, -1.15, 1.15))
    stencil_w = jax.random.uniform(key_w, (26,), jnp.float32, 0.5, 1.5) / 26.0
    omega_relax = jax.random.uniform(key_o, (SWEEPS,), jnp.float32, 0.6, 0.95)
    return {'u_init': u_init, 'source': source, 'kappa_cell': kappa_cell, 'stencil_w': stencil_w, 'omega_relax': omega_relax}


def reference(u_init, source, kappa_cell, stencil_w, omega_relax):
    offsets = stencil_offsets()
    diagonal = jnp.zeros_like(kappa_cell)
    for term_idx, offset in enumerate(offsets):
        diagonal = diagonal + 0.5 * stencil_w[term_idx] * (kappa_cell + neighbour(kappa_cell, offset))

    def jacobi_sweep(field_u, omega_k):
        applied = jnp.zeros_like(field_u)
        for term_idx, offset in enumerate(offsets):
            coupling = 0.5 * stencil_w[term_idx] * (kappa_cell + neighbour(kappa_cell, offset))
            applied = applied + coupling * (field_u - neighbour(field_u, offset))
        residual = source - applied
        norm_k = jnp.sqrt(jnp.sum(residual * residual) / CELLS)
        return field_u + omega_k * residual / diagonal, norm_k

    u_final, res_norms = lax.scan(jacobi_sweep, u_init, omega_relax)
    return u_final, res_norms
```

```python
import jax
import jax.numpy as jnp
from jax import lax
from jax.experimental import pallas as pl
from jax.experimental.pallas import tpu as pltpu
from jax.sharding import PartitionSpec as P

MESH = pl.DeviceIdType.MESH
F32 = jnp.float32
DEPTH = 8
BLOCKS = 4
SWEEPS = 32
CELLS = 64 * 64 * 64
OFFSETS = [(a, b, c) for a in (-1, 0, 1) for b in (-1, 0, 1) for c in (-1, 0, 1) if (a, b, c) != (0, 0, 0)]
TERM = {o: n for n, o in enumerate(OFFSETS)}


def kernel(u_ref, f_ref, k_ref, w_ref, om_ref, out_ref, rho_ref,
           pack, recv_own, kap, fld, coef, src_own, src_div, inv, diag, halo, sums, part, back, back_recv,
           own_send, own_recv, ring_send, ring_recv, back_send, back_recv_sem, sum_send, sum_recv):
    xc = lax.axis_index('x')
    yc = lax.axis_index('y')
    zc = lax.axis_index('z')
    me = 4 * zc + 2 * yc + xc
    turn = (yc + zc) % 2
    my_l = xc + turn * (3 - 2 * xc)
    my_q = 2 * xc + zc

    def slab_device(slab_y, slab_l):
        t = slab_l // 2
        return {'batch': 0, 'z': (slab_y + t) % 2, 'y': slab_y, 'x': slab_l + t * (3 - 2 * slab_l)}

    def ring_device(step):
        s = (4 * yc + my_l + step + 8) % 8
        return slab_device(s // 4, s % 4)

    def device(i):
        return {'batch': 0, 'z': i // 4, 'y': (i // 2) % 2, 'x': i % 2}

    lane = lax.broadcasted_iota(jnp.int32, (32, 128), 1) % 64
    is_first = lane == 0
    is_last = lane == 63

    barrier = pltpu.get_barrier_semaphore()
    for r in range(1, 8):
        pl.semaphore_signal(barrier, inc=1, device_id=device((me + r) % 8), device_id_type=MESH)

    def pack_array(a, ref):
        def body(i, _):
            rows = [ref[pl.ds(4 * i + m, 32, stride=32), :] for m in range(4)]
            pack[a, i] = jnp.concatenate(rows, axis=1)
            return 0
        lax.fori_loop(0, 8, body, 0)

    def own_copy(a, r):
        dest = (my_l + r) % 4
        return pltpu.make_async_remote_copy(
            src_ref=pack.at[a, pl.ds(2 * dest, 2)], dst_ref=recv_own.at[a, my_q],
            send_sem=own_send.at[a, r - 1], recv_sem=own_recv.at[a, r - 1],
            device_id=slab_device(yc, dest), device_id_type=MESH)

    def send_own(a):
        for r in range(1, 4):
            own_copy(a, r).start()
        recv_own[a, my_q] = pack[a, pl.ds(2 * my_l, 2)]

    def put(dst, plane, v):
        v_next = jnp.where(is_last, pltpu.roll(v, 63, 1), pltpu.roll(v, 127, 1))
        v_prev = jnp.where(is_first, pltpu.roll(v, 65, 1), pltpu.roll(v, 1, 1))
        for ver, val in ((0, v_prev), (1, v), (2, v_next)):
            dst[ver, plane, 8:40, :] = val
            dst[ver, plane, 7:8, :] = pltpu.roll(val[24:32], 64, 1)[7:8]
            dst[ver, plane, 40:41, :] = pltpu.roll(val[0:8], 64, 1)[0:1]

    def wait_own(a):
        for r in range(1, 4):
            own_copy(a, r).wait_recv()

    def unpack_own(a, store):
        def body(yy, _):
            for m in range(4):
                v = jnp.concatenate([recv_own[a, q, yy, :, 32 * m:32 * m + 32] for q in range(4)], axis=1)
                store(4 * yy + m, v)
            return 0
        lax.fori_loop(0, 2, body, 0)

    def ring_copy(e, src, side):
        return pltpu.make_async_remote_copy(
            src_ref=src, dst_ref=halo.at[e, side],
            send_sem=ring_send.at[e, side], recv_sem=ring_recv.at[e, side],
            device_id=ring_device(1 if side == 0 else -1), device_id_type=MESH)

    def u_source():
        return fld.at[0, 1, pl.ds(8, 8), pl.ds(8, 32), :]

    pack_array(0, k_ref)
    pl.semaphore_wait(barrier, 7)
    send_own(0)
    pack_array(1, u_ref)
    send_own(1)
    pack_array(2, f_ref)
    send_own(2)

    kap_src = kap.at[1, pl.ds(8, 8), pl.ds(8, 32), :]
    wait_own(0)
    unpack_own(0, lambda y, v: put(kap, 8 + y, v))
    for side in range(2):
        ring_copy(0, kap_src, side).start()
    wait_own(1)
    unpack_own(1, lambda y, v: put(fld.at[0], 8 + y, v))
    for side in range(2):
        ring_copy(2, u_source(), side).start()
    wait_own(2)

    def store_f(y, v):
        src_own[y] = v
    unpack_own(2, store_f)
    for side in range(2):
        ring_copy(1, src_own, side).start()

    def unpack_halo(e, dst):
        for side in range(2):
            def body(j, _):
                put(dst, 16 * side + j, halo[e, side, j])
                return 0
            lax.fori_loop(0, 8, body, 0)

    for side in range(2):
        ring_copy(0, kap_src, side).wait()
    unpack_halo(0, kap)

    half_w = [0.5 * w_ref[n] for n in range(26)]

    def coef_plane(p, _):
        for g in range(4):
            rows = pl.ds(8 * g, 8)
            center = kap[1, p, 8 + 8 * g:16 + 8 * g, :]
            terms = []
            total = None
            for n, (ox, oy, oz) in enumerate(OFFSETS):
                near = kap[oz + 1, p + oy, 8 + 8 * g + ox:16 + 8 * g + ox, :]
                c = half_w[n] * (center + near)
                terms.append(c)
                total = c if total is None else total + c
            recip = 1.0 / total
            inv[p, rows, :] = recip
            diag[p, rows, :] = total
            for n in range(26):
                coef[n, p, rows, :] = terms[n] * recip
        return 0
    lax.fori_loop(1, 23, coef_plane, 0)

    for side in range(2):
        ring_copy(1, src_own, side).wait()

    def scale_f(j, _):
        src_div[j] = halo[1, 0, j] * inv[j]
        src_div[8 + j] = src_own[j] * inv[8 + j]
        src_div[16 + j] = halo[1, 1, j] * inv[16 + j]
        return 0
    lax.fori_loop(0, 8, scale_f, 0)

    def load9(b, plane):
        return [[fld[b, oz + 1, plane, 8 + ox:40 + ox, :] for oz in (-1, 0, 1)] for ox in (-1, 0, 1)]

    def gather(acc, near, oy, plane):
        for ox in (-1, 0, 1):
            for oz in (-1, 0, 1):
                if (ox, oy, oz) == (0, 0, 0):
                    acc = acc - near[1][1]
                else:
                    acc = acc + coef[TERM[(ox, oy, oz)], plane] * near[ox + 1][oz + 1]
        return acc

    def segment(b, lo, hi, om, norm, carry):
        def body(m, carry):
            acc0, acc1, total = carry
            near = load9(b, m + 1)
            acc0 = gather(acc0, near, 1, m)
            acc1 = gather(acc1, near, 0, m + 1)
            acc2 = gather(src_div[m + 2], near, -1, m + 2)
            put(fld.at[1 - b], m, fld[b, 1, m, 8:40, :] + om * acc0)
            if norm:
                r = acc0 * diag[m]
                total = total + r * r
            return acc1, acc2, total
        return lax.fori_loop(lo, hi, body, carry)

    def block(blk, _):
        e = 2 + blk
        for side in range(2):
            ring_copy(e, u_source(), side).wait()
        unpack_halo(e, fld.at[0])

        def sweep(i, _):
            b = i % 2
            k = DEPTH * blk + i
            om = om_ref[k]
            lo = 1 + i
            near = load9(b, lo - 1)
            acc0 = gather(src_div[lo], near, -1, lo)
            near = load9(b, lo)
            acc0 = gather(acc0, near, 0, lo)
            acc1 = gather(src_div[lo + 1], near, -1, lo + 1)
            carry = (acc0, acc1, jnp.zeros((32, 128), F32))
            carry = segment(b, lo, 8, om, False, carry)
            carry = segment(b, 8, 16, om, True, carry)
            t = carry[2]
            sums[k] = t[0:8] + t[8:16] + t[16:24] + t[24:32]
            segment(b, 16, 23 - i, om, False, carry)
            return 0
        lax.fori_loop(0, DEPTH, sweep, 0)

        @pl.when(blk < BLOCKS - 1)
        def _():
            for side in range(2):
                ring_copy(e + 1, u_source(), side).start()
        return 0
    lax.fori_loop(0, BLOCKS, block, 0)

    def sum_copy(r):
        return pltpu.make_async_remote_copy(
            src_ref=part.at[8], dst_ref=part.at[me], send_sem=sum_send.at[r - 1], recv_sem=sum_recv.at[r - 1],
            device_id=device((me + r) % 8), device_id_type=MESH)

    flat = jnp.sum(sums[...], axis=1)
    flat = jnp.concatenate([flat, jnp.zeros((96, 128), F32)], axis=0)
    mine = jnp.sum(flat.T, axis=0, keepdims=True)
    mine = jnp.broadcast_to(mine, (8, 128))
    part[8] = mine
    part[me] = mine
    for r in range(1, 8):
        sum_copy(r).start()

    def back_copy(r):
        q = (my_q + r) % 4
        return pltpu.make_async_remote_copy(
            src_ref=back.at[q], dst_ref=back_recv.at[my_l], send_sem=back_send.at[r - 1], recv_sem=back_recv_sem.at[r - 1],
            device_id={'batch': 0, 'z': q % 2, 'y': yc, 'x': q // 2}, device_id_type=MESH)

    for yy in range(2):
        planes = [fld[0, 1, 8 + 4 * yy + m, 8:40, :] for m in range(4)]
        for q in range(4):
            back[q, yy] = jnp.concatenate([v[:, 32 * q:32 * q + 32] for v in planes], axis=1)
    for r in range(1, 4):
        back_copy(r).start()
    back_recv[my_l] = back[my_q]
    for r in range(1, 4):
        back_copy(r).wait()

    def unpack_back(i, _):
        v = back_recv[i // 2, i % 2]
        for m in range(4):
            out_ref[pl.ds(4 * i + m, 32, stride=32), :] = v[:, 32 * m:32 * m + 32]
        return 0
    lax.fori_loop(0, 8, unpack_back, 0)

    for r in range(1, 8):
        sum_copy(r).wait()
    total = part[0]
    for i in range(1, 8):
        total = total + part[i]
    rho_ref[...] = jnp.sqrt(total / CELLS)[0:1, 0:32]

    for a in range(3):
        for r in range(1, 4):
            own_copy(a, r).wait_send()


def solution(mesh):
    field_spec = P(('batch', 'x'), 'y', 'z')

    def local(u, f, kappa, w, om):
        vmem = pl.BlockSpec(memory_space=pltpu.VMEM)
        smem = pl.BlockSpec(memory_space=pltpu.SMEM)
        dma = pltpu.SemaphoreType.DMA
        out, rho = pl.pallas_call(
            kernel,
            out_shape=(jax.ShapeDtypeStruct((1024, 32), F32), jax.ShapeDtypeStruct((1, 32), F32)),
            in_specs=[vmem, vmem, vmem, smem, smem],
            out_specs=(vmem, vmem),
            scratch_shapes=[
                pltpu.VMEM((3, 8, 32, 128), F32),
                pltpu.VMEM((3, 4, 2, 32, 128), F32),
                pltpu.VMEM((3, 24, 48, 128), F32),
                pltpu.VMEM((2, 3, 24, 48, 128), F32),
                pltpu.VMEM((26, 26, 32, 128), F32),
                pltpu.VMEM((8, 32, 128), F32),
                pltpu.VMEM((26, 32, 128), F32),
                pltpu.VMEM((24, 32, 128), F32),
                pltpu.VMEM((24, 32, 128), F32),
                pltpu.VMEM((6, 2, 8, 32, 128), F32),
                pltpu.VMEM((32, 8, 128), F32),
                pltpu.VMEM((9, 8, 128), F32),
                pltpu.VMEM((4, 2, 32, 128), F32),
                pltpu.VMEM((4, 2, 32, 128), F32),
                dma((3, 3)), dma((3, 3)), dma((6, 2)), dma((6, 2)), dma((3,)), dma((3,)), dma((7,)), dma((7,)),
            ],
            compiler_params=pltpu.CompilerParams(collective_id=0, has_side_effects=True),
        )(u.reshape(1024, 32), f.reshape(1024, 32), kappa.reshape(1024, 32), w, om)
        return out.reshape(32, 32, 32), rho.reshape(32)

    return jax.shard_map(local, mesh=mesh, in_specs=(field_spec, field_spec, field_spec, P(), P()),
                         out_specs=(field_spec, P('batch')), check_vma=False)
```

```python
import jax
import jax.numpy as jnp
from jax import lax
from jax.experimental import pallas as pl
from jax.experimental.pallas import tpu as pltpu
from jax.sharding import PartitionSpec as P

MESH = pl.DeviceIdType.MESH
F32 = jnp.float32
DEPTH = 8
BLOCKS = 4
SWEEPS = 32
CELLS = 64 * 64 * 64
OFFSETS = [(a, b, c) for a in (-1, 0, 1) for b in (-1, 0, 1) for c in (-1, 0, 1) if (a, b, c) != (0, 0, 0)]
TERM = {o: n for n, o in enumerate(OFFSETS)}


def kernel(u_ref, f_ref, k_ref, w_ref, om_ref, out_ref, rho_ref,
           pack, recv_own, kap, fld_a, fld_b, coef, src_own, src_div, inv, diag, halo, sums, part, back, back_recv,
           own_send, own_recv, ring_send, ring_recv, back_send, back_recv_sem, sum_send, sum_recv):
    xc = lax.axis_index('x')
    yc = lax.axis_index('y')
    zc = lax.axis_index('z')
    me = 4 * zc + 2 * yc + xc
    turn = (yc + zc) % 2
    my_l = xc + turn * (3 - 2 * xc)
    my_q = 2 * xc + zc

    def slab_device(slab_y, slab_l):
        t = slab_l // 2
        return {'batch': 0, 'z': (slab_y + t) % 2, 'y': slab_y, 'x': slab_l + t * (3 - 2 * slab_l)}

    def ring_device(step):
        s = (4 * yc + my_l + step + 8) % 8
        return slab_device(s // 4, s % 4)

    def device(i):
        return {'batch': 0, 'z': i // 4, 'y': (i // 2) % 2, 'x': i % 2}

    lane = lax.broadcasted_iota(jnp.int32, (32, 128), 1) % 64
    is_first = lane == 0
    is_last = lane == 63

    barrier = pltpu.get_barrier_semaphore()
    for r in range(1, 8):
        pl.semaphore_signal(barrier, inc=1, device_id=device((me + r) % 8), device_id_type=MESH)

    def pack_array(a, ref):
        def body(i, _):
            rows = [ref[pl.ds(4 * i + m, 32, stride=32), :] for m in range(4)]
            pack[a, i] = jnp.concatenate(rows, axis=1)
            return 0
        lax.fori_loop(0, 8, body, 0)

    def own_copy(a, r):
        dest = (my_l + r) % 4
        return pltpu.make_async_remote_copy(
            src_ref=pack.at[a, pl.ds(2 * dest, 2)], dst_ref=recv_own.at[a, my_q],
            send_sem=own_send.at[a, r - 1], recv_sem=own_recv.at[a, r - 1],
            device_id=slab_device(yc, dest), device_id_type=MESH)

    def send_own(a):
        for r in range(1, 4):
            own_copy(a, r).start()
        recv_own[a, my_q] = pack[a, pl.ds(2 * my_l, 2)]

    def row(ver, first):
        return slice(40 * ver + first, 40 * ver + first + 32)

    def put(dst, plane, v):
        r1, r63, r65, r127 = (pltpu.roll(v, s, 1) for s in (1, 63, 65, 127))
        dst[plane, row(1, 8), :] = v
        dst[plane, row(0, 8), :] = jnp.where(is_first, r65, r1)
        dst[plane, row(2, 8), :] = jnp.where(is_last, r63, r127)
        low, high, first, last = slice(0, 8), slice(24, 32), is_first[0:8], is_last[0:8]
        for part, src, dest in ((high, 7, 7), (low, 0, 40)):
            swap = pltpu.roll(v[part], 64, 1)
            prev = jnp.where(first, r1[part], r65[part])
            nxt = jnp.where(last, r127[part], r63[part])
            for ver, val in ((0, prev), (1, swap), (2, nxt)):
                dst[plane, 40 * ver + dest:40 * ver + dest + 1, :] = val[src:src + 1]

    def wait_own(a):
        for r in range(1, 4):
            own_copy(a, r).wait_recv()

    def unpack_own(a, store):
        def body(yy, _):
            for m in range(4):
                v = jnp.concatenate([recv_own[a, q, yy, :, 32 * m:32 * m + 32] for q in range(4)], axis=1)
                store(4 * yy + m, v)
            return 0
        lax.fori_loop(0, 2, body, 0)

    def ring_copy(e, src, side):
        return pltpu.make_async_remote_copy(
            src_ref=src, dst_ref=halo.at[e, side],
            send_sem=ring_send.at[e, side], recv_sem=ring_recv.at[e, side],
            device_id=ring_device(1 if side == 0 else -1), device_id_type=MESH)

    def u_source():
        return fld_a.at[pl.ds(8, 8), pl.ds(48, 32), :]

    pack_array(0, k_ref)
    pl.semaphore_wait(barrier, 7)
    send_own(0)
    pack_array(1, u_ref)
    send_own(1)
    pack_array(2, f_ref)
    send_own(2)

    kap_src = kap.at[pl.ds(8, 8), pl.ds(48, 32), :]
    wait_own(0)
    unpack_own(0, lambda y, v: put(kap, 8 + y, v))
    for side in range(2):
        ring_copy(0, kap_src, side).start()
    wait_own(1)
    unpack_own(1, lambda y, v: put(fld_a, 8 + y, v))
    for side in range(2):
        ring_copy(2, u_source(), side).start()
    wait_own(2)

    def store_f(y, v):
        src_own[y] = v
    unpack_own(2, store_f)
    for side in range(2):
        ring_copy(1, src_own, side).start()

    def unpack_halo(e, dst):
        for side in range(2):
            def body(j, _):
                for m in range(4):
                    put(dst, 16 * side + 4 * j + m, halo[e, side, 4 * j + m])
                return 0
            lax.fori_loop(0, 2, body, 0)

    for side in range(2):
        ring_copy(0, kap_src, side).wait()
    unpack_halo(0, kap)

    half_w = [0.5 * w_ref[n] for n in range(26)]

    def coef_plane(p, _):
        for g in range(4):
            rows = pl.ds(8 * g, 8)
            center = kap[p, 48 + 8 * g:56 + 8 * g, :]
            terms = []
            total = None
            for n, (ox, oy, oz) in enumerate(OFFSETS):
                first = 40 * (oz + 1) + 8 + 8 * g + ox
                near = kap[p + oy, first:first + 8, :]
                c = half_w[n] * (center + near)
                terms.append(c)
                total = c if total is None else total + c
            recip = 1.0 / total
            inv[p, rows, :] = recip
            diag[p, rows, :] = jnp.where(jnp.logical_and(p >= 8, p < 16), total, 0.0)
            for n in range(26):
                coef[p, g, 8 * n:8 * n + 8, :] = terms[n] * recip
        return 0
    lax.fori_loop(1, 23, coef_plane, 0)

    for side in range(2):
        ring_copy(1, src_own, side).wait()

    def scale_f(j, _):
        src_div[j] = halo[1, 0, j] * inv[j]
        src_div[8 + j] = src_own[j] * inv[8 + j]
        src_div[16 + j] = halo[1, 1, j] * inv[16 + j]
        return 0
    lax.fori_loop(0, 8, scale_f, 0)

    def load9(ref, plane):
        return [[ref[plane, row(oz + 1, 8 + ox), :] for oz in (-1, 0, 1)] for ox in (-1, 0, 1)]

    def gather(acc, near, oy, plane):
        for ox in (-1, 0, 1):
            for oz in (-1, 0, 1):
                if (ox, oy, oz) == (0, 0, 0):
                    acc = acc - near[1][1]
                else:
                    n = TERM[(ox, oy, oz)]
                    c = jnp.concatenate([coef[plane, g, 8 * n:8 * n + 8, :] for g in range(4)], axis=0)
                    acc = acc + c * near[ox + 1][oz + 1]
        return acc

    def step(src, dst, om, m, carry):
        acc0, acc1, total = carry
        near = load9(src, m + 1)
        acc0 = gather(acc0, near, 1, m)
        acc1 = gather(acc1, near, 0, m + 1)
        acc2 = gather(src_div[m + 2], near, -1, m + 2)
        dst[m, row(1, 8), :] = src[m, row(1, 8), :] + om * acc0
        r = acc0 * diag[m]
        r = r * r
        total = total + ((r[0:8] + r[8:16]) + (r[16:24] + r[24:32]))
        return acc1, acc2, total

    def finish(dst, m):
        put(dst, m, dst[m, row(1, 8), :])

    def sweep(src, dst, i, k):
        om = om_ref[k]
        lo = 1 + i
        near = load9(src, lo - 1)
        acc0 = gather(src_div[lo], near, -1, lo)
        near = load9(src, lo)
        acc0 = gather(acc0, near, 0, lo)
        acc1 = gather(src_div[lo + 1], near, -1, lo + 1)
        carry = (acc0, acc1, jnp.zeros((8, 128), F32))
        if i % 2 == 0:
            carry = step(src, dst, om, lo, carry)
            carry = step(src, dst, om, lo + 1, carry)
            lo = lo + 2

        def body(t, carry):
            m = lo + 4 * t
            finish(dst, m - 2)
            finish(dst, m - 1)
            carry = step(src, dst, om, m, carry)
            carry = step(src, dst, om, m + 1, carry)
            finish(dst, m)
            finish(dst, m + 1)
            carry = step(src, dst, om, m + 2, carry)
            return step(src, dst, om, m + 3, carry)
        carry = lax.fori_loop(0, (23 - i - lo) // 4, body, carry)
        sums[k] = carry[2]
        finish(dst, 21 - i)
        finish(dst, 22 - i)

    def block(blk, _):
        e = 2 + blk
        for side in range(2):
            ring_copy(e, u_source(), side).wait()
        unpack_halo(e, fld_a)
        for i in range(DEPTH):
            src, dst = (fld_a, fld_b) if i % 2 == 0 else (fld_b, fld_a)
            sweep(src, dst, i, DEPTH * blk + i)

        @pl.when(blk < BLOCKS - 1)
        def _():
            for side in range(2):
                ring_copy(e + 1, u_source(), side).start()
        return 0
    lax.fori_loop(0, BLOCKS, block, 0)

    def sum_copy(r):
        return pltpu.make_async_remote_copy(
            src_ref=part.at[8], dst_ref=part.at[me], send_sem=sum_send.at[r - 1], recv_sem=sum_recv.at[r - 1],
            device_id=device((me + r) % 8), device_id_type=MESH)

    flat = jnp.sum(sums[...], axis=1)
    flat = jnp.concatenate([flat, jnp.zeros((96, 128), F32)], axis=0)
    mine = jnp.sum(flat.T, axis=0, keepdims=True)
    mine = jnp.broadcast_to(mine, (8, 128))
    part[8] = mine
    part[me] = mine
    for r in range(1, 8):
        sum_copy(r).start()

    def back_copy(r):
        q = (my_q + r) % 4
        return pltpu.make_async_remote_copy(
            src_ref=back.at[q], dst_ref=back_recv.at[my_l], send_sem=back_send.at[r - 1], recv_sem=back_recv_sem.at[r - 1],
            device_id={'batch': 0, 'z': q % 2, 'y': yc, 'x': q // 2}, device_id_type=MESH)

    for yy in range(2):
        planes = [fld_a[8 + 4 * yy + m, row(1, 8), :] for m in range(4)]
        for q in range(4):
            back[q, yy] = jnp.concatenate([v[:, 32 * q:32 * q + 32] for v in planes], axis=1)
    for r in range(1, 4):
        back_copy(r).start()
    back_recv[my_l] = back[my_q]
    for r in range(1, 4):
        back_copy(r).wait()

    def unpack_back(i, _):
        v = back_recv[i // 2, i % 2]
        for m in range(4):
            out_ref[pl.ds(4 * i + m, 32, stride=32), :] = v[:, 32 * m:32 * m + 32]
        return 0
    lax.fori_loop(0, 8, unpack_back, 0)

    for r in range(1, 8):
        sum_copy(r).wait()
    total = part[0]
    for i in range(1, 8):
        total = total + part[i]
    rho_ref[...] = jnp.sqrt(total / CELLS)[0:1, 0:32]

    for a in range(3):
        for r in range(1, 4):
            own_copy(a, r).wait_send()


def solution(mesh):
    field_spec = P(('batch', 'x'), 'y', 'z')

    def local(u, f, kappa, w, om):
        vmem = pl.BlockSpec(memory_space=pltpu.VMEM)
        smem = pl.BlockSpec(memory_space=pltpu.SMEM)
        dma = pltpu.SemaphoreType.DMA
        out, rho = pl.pallas_call(
            kernel,
            out_shape=(jax.ShapeDtypeStruct((1024, 32), F32), jax.ShapeDtypeStruct((1, 32), F32)),
            in_specs=[vmem, vmem, vmem, smem, smem],
            out_specs=(vmem, vmem),
            scratch_shapes=[
                pltpu.VMEM((3, 8, 32, 128), F32),
                pltpu.VMEM((3, 4, 2, 32, 128), F32),
                pltpu.VMEM((24, 128, 128), F32),
                pltpu.VMEM((24, 128, 128), F32),
                pltpu.VMEM((24, 128, 128), F32),
                pltpu.VMEM((26, 4, 208, 128), F32),
                pltpu.VMEM((8, 32, 128), F32),
                pltpu.VMEM((26, 32, 128), F32),
                pltpu.VMEM((24, 32, 128), F32),
                pltpu.VMEM((24, 32, 128), F32),
                pltpu.VMEM((6, 2, 8, 32, 128), F32),
                pltpu.VMEM((32, 8, 128), F32),
                pltpu.VMEM((9, 8, 128), F32),
                pltpu.VMEM((4, 2, 32, 128), F32),
                pltpu.VMEM((4, 2, 32, 128), F32),
                dma((3, 3)), dma((3, 3)), dma((6, 2)), dma((6, 2)), dma((3,)), dma((3,)), dma((7,)), dma((7,)),
            ],
            compiler_params=pltpu.CompilerParams(collective_id=0, has_side_effects=True),
        )(u.reshape(1024, 32), f.reshape(1024, 32), kappa.reshape(1024, 32), w, om)
        return out.reshape(32, 32, 32), rho.reshape(32)

    return jax.shard_map(local, mesh=mesh, in_specs=(field_spec, field_spec, field_spec, P(), P()),
                         out_specs=(field_spec, P('batch')), check_vma=False)
```

```python
import jax
import jax.numpy as jnp
from jax import lax
from jax.experimental import pallas as pl
from jax.experimental.pallas import tpu as pltpu
from jax.sharding import PartitionSpec as P

MESH = pl.DeviceIdType.MESH
F32 = jnp.float32
DEPTH = 8
BLOCKS = 4
SWEEPS = 32
CELLS = 64 * 64 * 64
OFFSETS = [(a, b, c) for a in (-1, 0, 1) for b in (-1, 0, 1) for c in (-1, 0, 1) if (a, b, c) != (0, 0, 0)]
TERM = {o: n for n, o in enumerate(OFFSETS)}


def kernel(u_ref, f_ref, k_ref, w_ref, om_ref, out_ref, rho_ref,
           pack, recv_own, kap, fld_a, fld_b, coef, src_own, src_div, inv, diag, stage, halo, sums, psum, back, back_recv,
           own_send, own_recv, ring_send, ring_recv, back_send, back_recv_sem, sum_send, sum_recv):
    xc = lax.axis_index('x')
    yc = lax.axis_index('y')
    zc = lax.axis_index('z')
    me = 4 * zc + 2 * yc + xc
    turn = (yc + zc) % 2
    my_l = xc + turn * (3 - 2 * xc)
    my_q = 2 * xc + zc

    def slab_device(slab_y, slab_l):
        t = slab_l // 2
        return {'batch': 0, 'z': (slab_y + t) % 2, 'y': slab_y, 'x': slab_l + t * (3 - 2 * slab_l)}

    def ring_device(step):
        s = (4 * yc + my_l + step + 8) % 8
        return slab_device(s // 4, s % 4)

    def device(i):
        return {'batch': 0, 'z': i // 4, 'y': (i // 2) % 2, 'x': i % 2}

    lane = lax.broadcasted_iota(jnp.int32, (1, 32, 128), 2) % 64
    is_first = lane == 0
    is_last = lane == 63

    barrier = pltpu.get_barrier_semaphore()
    for r in range(1, 8):
        pl.semaphore_signal(barrier, inc=1, device_id=device((me + r) % 8), device_id_type=MESH)

    def pack_array(a, ref):
        def body(i, _):
            rows = [ref[pl.ds(4 * i + m, 32, stride=32), :] for m in range(4)]
            pack[a, i] = jnp.concatenate(rows, axis=1)
            return 0
        lax.fori_loop(0, 8, body, 0)

    def own_copy(a, r):
        dest = (my_l + r) % 4
        return pltpu.make_async_remote_copy(
            src_ref=pack.at[a, pl.ds(2 * dest, 2)], dst_ref=recv_own.at[a, my_q],
            send_sem=own_send.at[a, r - 1], recv_sem=own_recv.at[a, r - 1],
            device_id=slab_device(yc, dest), device_id_type=MESH)

    def send_own(a):
        for r in range(1, 4):
            own_copy(a, r).start()
        recv_own[a, my_q] = pack[a, pl.ds(2 * my_l, 2)]

    def row(ver, first):
        return slice(40 * ver + first, 40 * ver + first + 32)

    def put(dst, plane, v):
        planes = pl.ds(plane, v.shape[0])
        r1, r63, r65, r127 = (pltpu.roll(v, s, 2) for s in (1, 63, 65, 127))
        dst[planes, row(1, 8), :] = v
        dst[planes, row(0, 8), :] = jnp.where(is_first, r65, r1)
        dst[planes, row(2, 8), :] = jnp.where(is_last, r63, r127)
        first, last = is_first[:, 0:8], is_last[:, 0:8]
        for rows, src, dest in ((slice(24, 32), 7, 7), (slice(0, 8), 0, 40)):
            swap = pltpu.roll(v[:, rows], 64, 2)
            prev = jnp.where(first, r1[:, rows], r65[:, rows])
            nxt = jnp.where(last, r127[:, rows], r63[:, rows])
            for ver, val in ((0, prev), (1, swap), (2, nxt)):
                dst[planes, 40 * ver + dest:40 * ver + dest + 1, :] = val[:, src:src + 1]

    def wait_own(a):
        for r in range(1, 4):
            own_copy(a, r).wait_recv()

    def unpack_own(a, store):
        def body(yy, _):
            for m in range(4):
                v = jnp.concatenate([recv_own[a, q, yy, :, 32 * m:32 * m + 32] for q in range(4)], axis=1)
                store(4 * yy + m, v)
            return 0
        lax.fori_loop(0, 2, body, 0)

    def ring_copy(e, src, dst, side, part):
        first = 4 * (1 - part) if side == 0 else 4 * part
        return pltpu.make_async_remote_copy(
            src_ref=src(first), dst_ref=dst(side, first),
            send_sem=ring_send.at[e, side, part], recv_sem=ring_recv.at[e, side, part],
            device_id=ring_device(1 if side == 0 else -1), device_id_type=MESH)

    def halo_dst(e):
        return lambda side, first: halo.at[e, side, pl.ds(first, 4)]

    def kap_copy(side, part):
        return ring_copy(0, lambda first: kap.at[pl.ds(8 + first, 4), pl.ds(48, 32), :], halo_dst(0), side, part)

    def f_copy(side, part):
        return ring_copy(1, lambda first: src_own.at[pl.ds(8 + first, 4)],
                         lambda side, first: src_own.at[pl.ds(16 * side + first, 4)], side, part)

    def u_copy(e, side, part):
        return ring_copy(e, lambda first: stage.at[pl.ds(first, 4)], halo_dst(e), side, part)

    PARTS = [(side, part) for part in range(2) for side in range(2)]

    def unpack_halo(e, dst, part):
        for side in range(2):
            j = 4 * (1 - part) if side == 0 else 4 * part
            put(dst, 16 * side + j, halo[e, side, j:j + 4])

    pack_array(0, k_ref)
    pl.semaphore_wait(barrier, 7)
    send_own(0)
    pack_array(1, u_ref)
    send_own(1)
    pack_array(2, f_ref)
    send_own(2)

    wait_own(0)
    unpack_own(0, lambda y, v: put(kap, 8 + y, v[None]))
    for side, part in PARTS:
        kap_copy(side, part).start()
    wait_own(1)

    def store_u(y, v):
        stage[y] = v
        put(fld_a, 8 + y, v[None])
    unpack_own(1, store_u)
    for side, part in PARTS:
        u_copy(2, side, part).start()
    wait_own(2)

    def store_f(y, v):
        src_own[8 + y] = v
    unpack_own(2, store_f)
    for side, part in PARTS:
        f_copy(side, part).start()

    half_w = [0.5 * w_ref[n] for n in range(26)]

    def coef_plane(p, _):
        for g in range(4):
            rows = pl.ds(8 * g, 8)
            center = kap[p, 48 + 8 * g:56 + 8 * g, :]
            terms = []
            total = None
            for n, (ox, oy, oz) in enumerate(OFFSETS):
                first = 40 * (oz + 1) + 8 + 8 * g + ox
                near = kap[p + oy, first:first + 8, :]
                c = half_w[n] * (center + near)
                terms.append(c)
                total = c if total is None else total + c
            recip = 1.0 / total
            inv[p, rows, :] = recip
            diag[p, rows, :] = total
            for n in range(26):
                coef[p, 40 * n + 8 * g:40 * n + 8 * g + 8, :] = terms[n] * recip
        return 0
    def scale_f(p, _):
        src_div[p] = src_own[p] * inv[p]
        return 0

    def coef_range(lo, hi):
        lax.fori_loop(lo, hi, coef_plane, 0)

    def scale_range(lo, hi):
        lax.fori_loop(lo, hi, scale_f, 0)

    sums[...] = jnp.zeros_like(sums)
    coef_range(9, 15)
    scale_range(9, 15)

    def strip(level, blk, lo, n):
        src, dst = (fld_a, fld_b) if level % 2 == 1 else (fld_b, fld_a)
        k = DEPTH * blk + level - 1
        acc = src_div[lo:lo + n] - src[lo:lo + n, row(1, 8), :]
        for ox in (-1, 0, 1):
            for oz in (-1, 0, 1):
                near = src[lo - 1:lo + n + 1, row(oz + 1, 8 + ox), :]
                for oy in (-1, 0, 1):
                    if (ox, oy, oz) != (0, 0, 0):
                        t = TERM[(ox, oy, oz)]
                        acc = acc + coef[lo:lo + n, 40 * t:40 * t + 32, :] * near[1 + oy:1 + oy + n]
        new = src[lo:lo + n, row(1, 8), :] + om_ref[k] * acc
        put(dst, lo, new)
        if level == DEPTH:
            stage[lo - 8:lo - 8 + n] = new
        a, b = max(lo, 8), min(lo + n, 16)
        if a < b:
            r = acc[a - lo:b - lo] * diag[a:b]
            r = jnp.sum(r * r, axis=0)
            sums[k] = sums[k] + ((r[0:8] + r[8:16]) + (r[16:24] + r[24:32]))

    def block(blk, _):
        e = 2 + blk
        for level, lo, n in ((1, 9, 3), (1, 12, 3), (2, 10, 2), (2, 12, 2), (3, 11, 2)):
            strip(level, blk, lo, n)

        for part in range(2):
            @pl.when(blk == 0)
            def _():
                for side in range(2):
                    kap_copy(side, part).wait()
                unpack_halo(0, kap, part)
                left, right = (5, 15) if part == 0 else (1, 19)
                coef_range(left, left + 4)
                coef_range(right, right + 4)
                for side in range(2):
                    f_copy(side, part).wait()
                scale_range(left, left + 4)
                scale_range(right, right + 4)
            for side in range(2):
                u_copy(e, side, part).wait()
            unpack_halo(e, fld_a, part)
            if part == 0:
                for level in range(1, 4):
                    strip(level, blk, 4 + level, 4)
                    strip(level, blk, 16 - level, 4)
                for level in range(4, 7):
                    strip(level, blk, 4 + level, 8 - level)
                    strip(level, blk, 12, 8 - level)
                strip(7, blk, 11, 2)
            else:
                for level in range(1, 9):
                    strip(level, blk, level, 4)
                    strip(level, blk, 20 - level, 4)

        @pl.when(blk < BLOCKS - 1)
        def _():
            for side, part in PARTS:
                u_copy(e + 1, side, part).start()
        return 0
    lax.fori_loop(0, BLOCKS, block, 0)

    def sum_copy(r):
        return pltpu.make_async_remote_copy(
            src_ref=psum.at[8], dst_ref=psum.at[me], send_sem=sum_send.at[r - 1], recv_sem=sum_recv.at[r - 1],
            device_id=device((me + r) % 8), device_id_type=MESH)

    flat = jnp.sum(sums[...], axis=1)
    flat = jnp.concatenate([flat, jnp.zeros((96, 128), F32)], axis=0)
    mine = jnp.sum(flat.T, axis=0, keepdims=True)
    mine = jnp.broadcast_to(mine, (8, 128))
    psum[8] = mine
    psum[me] = mine
    for r in range(1, 8):
        sum_copy(r).start()

    def back_copy(r):
        q = (my_q + r) % 4
        return pltpu.make_async_remote_copy(
            src_ref=back.at[q], dst_ref=back_recv.at[my_l], send_sem=back_send.at[r - 1], recv_sem=back_recv_sem.at[r - 1],
            device_id={'batch': 0, 'z': q % 2, 'y': yc, 'x': q // 2}, device_id_type=MESH)

    for yy in range(2):
        planes = [fld_a[8 + 4 * yy + m, row(1, 8), :] for m in range(4)]
        for q in range(4):
            back[q, yy] = jnp.concatenate([v[:, 32 * q:32 * q + 32] for v in planes], axis=1)
    for r in range(1, 4):
        back_copy(r).start()
    back_recv[my_l] = back[my_q]
    for r in range(1, 4):
        back_copy(r).wait()

    def unpack_back(i, _):
        v = back_recv[i // 2, i % 2]
        for m in range(4):
            out_ref[pl.ds(4 * i + m, 32, stride=32), :] = v[:, 32 * m:32 * m + 32]
        return 0
    lax.fori_loop(0, 8, unpack_back, 0)

    for r in range(1, 8):
        sum_copy(r).wait()
    total = psum[0]
    for i in range(1, 8):
        total = total + psum[i]
    rho_ref[...] = jnp.sqrt(total / CELLS)[0:1, 0:32]

    for a in range(3):
        for r in range(1, 4):
            own_copy(a, r).wait_send()


def solution(mesh):
    field_spec = P(('batch', 'x'), 'y', 'z')

    def local(u, f, kappa, w, om):
        vmem = pl.BlockSpec(memory_space=pltpu.VMEM)
        smem = pl.BlockSpec(memory_space=pltpu.SMEM)
        dma = pltpu.SemaphoreType.DMA
        out, rho = pl.pallas_call(
            kernel,
            out_shape=(jax.ShapeDtypeStruct((1024, 32), F32), jax.ShapeDtypeStruct((1, 32), F32)),
            in_specs=[vmem, vmem, vmem, smem, smem],
            out_specs=(vmem, vmem),
            scratch_shapes=[
                pltpu.VMEM((3, 8, 32, 128), F32),
                pltpu.VMEM((3, 4, 2, 32, 128), F32),
                pltpu.VMEM((24, 128, 128), F32),
                pltpu.VMEM((24, 128, 128), F32),
                pltpu.VMEM((24, 128, 128), F32),
                pltpu.VMEM((24, 1056, 128), F32),
                pltpu.VMEM((24, 32, 128), F32),
                pltpu.VMEM((24, 32, 128), F32),
                pltpu.VMEM((24, 32, 128), F32),
                pltpu.VMEM((24, 32, 128), F32),
                pltpu.VMEM((8, 32, 128), F32),
                pltpu.VMEM((6, 2, 8, 32, 128), F32),
                pltpu.VMEM((32, 8, 128), F32),
                pltpu.VMEM((9, 8, 128), F32),
                pltpu.VMEM((4, 2, 32, 128), F32),
                pltpu.VMEM((4, 2, 32, 128), F32),
                dma((3, 3)), dma((3, 3)), dma((6, 2, 2)), dma((6, 2, 2)), dma((3,)), dma((3,)), dma((7,)), dma((7,)),
            ],
            compiler_params=pltpu.CompilerParams(collective_id=0, has_side_effects=True),
        )(u.reshape(1024, 32), f.reshape(1024, 32), kappa.reshape(1024, 32), w, om)
        return out.reshape(32, 32, 32), rho.reshape(32)

    return jax.shard_map(local, mesh=mesh, in_specs=(field_spec, field_spec, field_spec, P(), P()),
                         out_specs=(field_spec, P('batch')), check_vma=False)
```

```python
import jax
import jax.numpy as jnp
from jax import lax
from jax.experimental import pallas as pl
from jax.experimental.pallas import tpu as pltpu
from jax.sharding import PartitionSpec as P

MESH = pl.DeviceIdType.MESH
F32 = jnp.float32
ROWS = 32
LANES = 128
BRICK = 1024
DEPTH = 8
BLOCKS = 4
CELLS = 64 * 64 * 64
OFFSETS = [(a, b, c) for a in (-1, 0, 1) for b in (-1, 0, 1) for c in (-1, 0, 1) if (a, b, c) != (0, 0, 0)]
TERM = {o: n for n, o in enumerate(OFFSETS)}


def kernel(u_ref, f_ref, k_ref, w_hbm, om_hbm, out_ref, rho_ref,
           w_ref, om_ref, bricks, brick_sem, pack, recv_own, kap, fld, coef, src_own, src_div, inv, diag, stage, halo, sums, psum, back, back_recv,
           own_send, own_recv, ring_send, ring_recv, back_send, back_recv_sem, sum_send, sum_recv):
    xc = lax.axis_index('x')
    yc = lax.axis_index('y')
    zc = lax.axis_index('z')
    me = 4 * zc + 2 * yc + xc
    turn = (yc + zc) % 2
    my_l = xc + turn * (3 - 2 * xc)
    my_q = 2 * xc + zc

    def slab_device(slab_y, slab_l):
        t = slab_l // 2
        return {'batch': 0, 'z': (slab_y + t) % 2, 'y': slab_y, 'x': slab_l + t * (3 - 2 * slab_l)}

    def ring_device(step):
        s = (4 * yc + my_l + step + 8) % 8
        return slab_device(s // 4, s % 4)

    def device(i):
        return {'batch': 0, 'z': i // 4, 'y': (i // 2) % 2, 'x': i % 2}

    even = lax.broadcasted_iota(jnp.int32, (1, 8, LANES), 2) % 2 == 0
    top = lax.broadcasted_iota(jnp.int32, (1, 8, LANES), 1) == 0
    lane_in = lax.broadcasted_iota(jnp.int32, (LANES, LANES), 0)
    lane_out = lax.broadcasted_iota(jnp.int32, (LANES, LANES), 1)
    weave = (lane_out == 2 * (lane_in % 64) + lane_in // 64).astype(F32)
    unweave = (lane_in == 2 * (lane_out % 64) + lane_out // 64).astype(F32)

    def move_lanes(v, matrix):
        return jnp.dot(v, matrix, precision=lax.Precision.HIGHEST, preferred_element_type=F32)

    barrier = pltpu.get_barrier_semaphore()
    for r in range(1, 8):
        pl.semaphore_signal(barrier, inc=1, device_id=device((me + r) % 8), device_id_type=MESH)

    loads = [pltpu.make_async_copy(ref, bricks.at[a], brick_sem.at[a]) for a, ref in enumerate((k_ref, u_ref, f_ref))]
    loads.append(pltpu.make_async_copy(w_hbm, w_ref, brick_sem.at[3]))
    loads.append(pltpu.make_async_copy(om_hbm, om_ref, brick_sem.at[4]))
    for load in loads:
        load.start()

    def pack_array(a):
        loads[a].wait()
        for i in range(8):
            rows = [bricks[a, pl.ds(4 * i + m, ROWS, stride=ROWS), :] for m in range(4)]
            pack[a, i] = jnp.concatenate(rows, axis=1)

    def own_copy(a, r):
        dest = (my_l + r) % 4
        return pltpu.make_async_remote_copy(
            src_ref=pack.at[a, pl.ds(2 * dest, 2)], dst_ref=recv_own.at[a, my_q],
            send_sem=own_send.at[a, r - 1], recv_sem=own_recv.at[a, r - 1],
            device_id=slab_device(yc, dest), device_id_type=MESH)

    def send_own(a):
        for r in range(1, 4):
            own_copy(a, r).start()
        recv_own[a, my_q] = pack[a, pl.ds(2 * my_l, 2)]

    def row(ver, first):
        return slice(40 * ver + first, 40 * ver + first + ROWS)

    def put(dst, plane, v):
        dst[pl.ds(plane, v.shape[0]), row(1, 8), :] = v
        put_turned(dst, plane, v)

    def put_turned(dst, plane, v):
        planes = pl.ds(plane, v.shape[0])
        dst[planes, row(0, 8), :] = pltpu.roll(v, 2, 2)
        dst[planes, row(2, 8), :] = pltpu.roll(v, 126, 2)
        edge = jnp.where(top, v[:, 0:8], v[:, 24:ROWS])
        r1, r3, r125, r127 = (pltpu.roll(edge, s, 2) for s in (1, 3, 125, 127))
        for ver, a, b in ((0, r1, r3), (1, r127, r1), (2, r125, r127)):
            swap = jnp.where(even, a, b)
            dst[planes, 40 * ver + 7:40 * ver + 8, :] = swap[:, 7:8]
            dst[planes, 40 * ver + 40:40 * ver + 41, :] = swap[:, 0:1]

    def wait_own(a):
        for r in range(1, 4):
            own_copy(a, r).wait_recv()

    def unpack_own(a, store):
        for yy in range(2):
            for m in range(4):
                v = jnp.concatenate([recv_own[a, q, yy, :, ROWS * m:ROWS * m + ROWS] for q in range(4)], axis=1)
                store(4 * yy + m, move_lanes(v, weave))

    def ring_copy(e, src, dst, side, part):
        first = 4 * (1 - part) if side == 0 else 4 * part
        return pltpu.make_async_remote_copy(
            src_ref=src(first), dst_ref=dst(side, first),
            send_sem=ring_send.at[e, side, part], recv_sem=ring_recv.at[e, side, part],
            device_id=ring_device(1 if side == 0 else -1), device_id_type=MESH)

    def halo_dst(e):
        return lambda side, first: halo.at[e, side, pl.ds(first, 4)]

    def kap_copy(side, part):
        return ring_copy(0, lambda first: kap.at[pl.ds(8 + first, 4), pl.ds(48, ROWS), :], halo_dst(0), side, part)

    def f_copy(side, part):
        return ring_copy(1, lambda first: src_own.at[pl.ds(8 + first, 4)],
                         lambda side, first: src_own.at[pl.ds(16 * side + first, 4)], side, part)

    def u_copy(e, side, part):
        return ring_copy(e, lambda first: stage.at[pl.ds(first, 4)], halo_dst(e), side, part)

    PARTS = [(side, part) for part in range(2) for side in range(2)]

    def unpack_halo(e, dst, part):
        for side in range(2):
            j = 4 * (1 - part) if side == 0 else 4 * part
            put(dst, 16 * side + j, halo[e, side, j:j + 4])

    pack_array(0)
    pl.semaphore_wait(barrier, 7)
    send_own(0)
    pack_array(1)
    send_own(1)
    pack_array(2)
    send_own(2)

    wait_own(0)
    unpack_own(0, lambda y, v: put(kap, 8 + y, v[None]))
    for side in range(2):
        kap_copy(side, 0).start()
    wait_own(1)

    def store_u(y, v):
        stage[y] = v
        put(fld, 8 + y, v[None])
    unpack_own(1, store_u)
    for side in range(2):
        u_copy(2, side, 0).start()
    for side in range(2):
        kap_copy(side, 1).start()
    wait_own(2)

    def store_f(y, v):
        src_own[8 + y] = v
    unpack_own(2, store_f)
    for side in range(2):
        f_copy(side, 0).start()
    for side in range(2):
        u_copy(2, side, 1).start()
    for side in range(2):
        f_copy(side, 1).start()

    loads[3].wait()
    loads[4].wait()
    half_w = [0.5 * w_ref[n] for n in range(26)]

    def coef_plane(p, _):
        for g in range(4):
            rows = pl.ds(8 * g, 8)
            center = kap[p, 48 + 8 * g:56 + 8 * g, :]
            terms = []
            total = None
            for n, (ox, oy, oz) in enumerate(OFFSETS):
                first = 40 * (oz + 1) + 8 + 8 * g + ox
                near = kap[p + oy, first:first + 8, :]
                c = half_w[n] * (center + near)
                terms.append(c)
                total = c if total is None else total + c
            recip = 1.0 / total
            inv[p, rows, :] = recip
            diag[p, rows, :] = jnp.where(jnp.logical_and(p >= 8, p < 16), total, 0.0)
            for n in range(26):
                coef[p, 40 * n + 8 * g:40 * n + 8 * g + 8, :] = terms[n] * recip
        return 0
    def scale_f(p, _):
        src_div[p] = src_own[p] * inv[p]
        return 0

    def coef_range(lo, hi):
        lax.fori_loop(lo, hi, coef_plane, 0)

    def scale_range(lo, hi):
        lax.fori_loop(lo, hi, scale_f, 0)

    sums[...] = jnp.zeros_like(sums)
    coef_range(9, 15)
    scale_range(9, 15)
    for part in range(2):
        for side in range(2):
            kap_copy(side, part).wait()
        unpack_halo(0, kap, part)
        coef_range(*((5, 9) if part == 0 else (1, 5)))
        coef_range(*((15, 19) if part == 0 else (19, 23)))

    def pair(level, first, second, n, before, blk):
        src, dst = (0, 24) if level % 2 == 1 else (24, 0)
        k = DEPTH * blk + level - 1
        om = om_ref[k]
        owned = first + n > 8

        def body(s, _):
            lo = first + s * (second - first)
            last = before + s * (dst + first - before)
            turned = fld[pl.ds(last, 4), row(1, 8), :]
            center = fld[pl.ds(src + lo, n), row(1, 8), :]
            acc = src_div[pl.ds(lo, n)] - center
            for ox in (-1, 0, 1):
                for oz in (-1, 0, 1):
                    near = fld[pl.ds(src + lo - 1, n + 2), row(oz + 1, 8 + ox), :]
                    for oy in (-1, 0, 1):
                        if (ox, oy, oz) != (0, 0, 0):
                            t = 40 * TERM[(ox, oy, oz)]
                            acc = acc + coef[pl.ds(lo, n), t:t + ROWS, :] * near[1 + oy:1 + oy + n]
            new = center + om * acc
            fld[pl.ds(dst + lo, n), row(1, 8), :] = new
            put_turned(fld, last, turned)
            if level == DEPTH:
                stage[pl.ds(lo - 8, n)] = new
            if owned:
                r = acc * diag[pl.ds(lo, n)]
                r = jnp.sum(r * r, axis=0)
                sums[k] = sums[k] + ((r[0:8] + r[8:16]) + (r[16:24] + r[24:ROWS]))
            return 0
        if first == second:
            body(0, 0)
        else:
            lax.fori_loop(0, 2, body, 0)
        return dst + second

    def flush(before):
        put_turned(fld, before, fld[pl.ds(before, 4), row(1, 8), :])
        return before

    def block(blk, _):
        e = 2 + blk
        before = 8
        for level, first, second, n in ((1, 9, 12, 3), (2, 10, 10, 4), (3, 11, 11, 2)):
            before = flush(pair(level, first, second, n, before, blk))
        for part in range(2):
            @pl.when(blk == 0)
            def _():
                left, right = (5, 15) if part == 0 else (1, 19)
                for side in range(2):
                    f_copy(side, part).wait()
                scale_range(left, left + 4)
                scale_range(right, right + 4)
            for side in range(2):
                u_copy(e, side, part).wait()
            unpack_halo(e, fld, part)
            if part == 0:
                for level in range(1, 4):
                    before = pair(level, 4 + level, 16 - level, 4, before, blk)
            else:
                for level in range(1, 9):
                    before = pair(level, level, 20 - level, 4, before, blk)
                    if level < 5:
                        first, second, n = ((8, 12, 4), (9, 12, 3), (10, 10, 4), (11, 11, 2))[level - 1]
                        before = pair(3 + level, first, second, n, before, blk)

        @pl.when(blk < BLOCKS - 1)
        def _():
            for side, part in PARTS:
                u_copy(e + 1, side, part).start()
            flush(before)
        return 0
    lax.fori_loop(0, BLOCKS, block, 0)

    def sum_copy(r):
        return pltpu.make_async_remote_copy(
            src_ref=psum.at[8], dst_ref=psum.at[me], send_sem=sum_send.at[r - 1], recv_sem=sum_recv.at[r - 1],
            device_id=device((me + r) % 8), device_id_type=MESH)

    def back_copy(r):
        q = (my_q + r) % 4
        return pltpu.make_async_remote_copy(
            src_ref=back.at[q], dst_ref=back_recv.at[my_l], send_sem=back_send.at[r - 1], recv_sem=back_recv_sem.at[r - 1],
            device_id={'batch': 0, 'z': q % 2, 'y': yc, 'x': q // 2}, device_id_type=MESH)

    for yy in range(2):
        planes = [move_lanes(fld[8 + 4 * yy + m, row(1, 8), :], unweave) for m in range(4)]
        for q in range(4):
            back[q, yy] = jnp.concatenate([v[:, ROWS * q:ROWS * q + ROWS] for v in planes], axis=1)
    for r in range(1, 4):
        back_copy(r).start()
    back_recv[my_l] = back[my_q]
    flat = jnp.sum(sums[...], axis=1)
    flat = jnp.concatenate([flat, jnp.zeros((96, LANES), F32)], axis=0)
    mine = jnp.sum(flat.T, axis=0, keepdims=True)
    mine = jnp.broadcast_to(mine, (8, LANES))
    psum[8] = mine
    psum[me] = mine
    for r in range(1, 8):
        sum_copy(r).start()

    for r in range(1, 4):
        back_copy(r).wait()
    out_ref[...] = back_recv[...]
    for r in range(1, 8):
        sum_copy(r).wait()
    total = psum[0]
    for i in range(1, 8):
        total = total + psum[i]
    rho_ref[...] = total

    for a in range(3):
        for r in range(1, 4):
            own_copy(a, r).wait_send()


def unpack_kernel(dense_ref, total_ref, out_ref, rho_ref):
    for i in range(8):
        v = dense_ref[i // 2, i % 2]
        for m in range(4):
            out_ref[pl.ds(4 * i + m, ROWS, stride=ROWS), :] = v[:, ROWS * m:ROWS * m + ROWS]
    rho_ref[...] = jnp.sqrt(total_ref[...] / CELLS)[0:1, 0:ROWS]


def solution(mesh):
    field_spec = P(('batch', 'x'), 'y', 'z')

    def local(u, f, kappa, w, om):
        vmem = pl.BlockSpec(memory_space=pltpu.VMEM)
        hbm = pl.BlockSpec(memory_space=pltpu.HBM)
        dma = pltpu.SemaphoreType.DMA
        dense, total = pl.pallas_call(
            kernel,
            out_shape=(pltpu.VMEM((4, 2, ROWS, LANES), F32), pltpu.VMEM((8, LANES), F32)),
            in_specs=[hbm] * 5,
            out_specs=(vmem, vmem),
            scratch_shapes=[
                pltpu.SMEM((26,), F32),
                pltpu.SMEM((ROWS,), F32),
                pltpu.VMEM((3, BRICK, ROWS), F32),
                dma((5,)),
                pltpu.VMEM((3, 8, ROWS, LANES), F32),
                pltpu.VMEM((3, 4, 2, ROWS, LANES), F32),
                pltpu.VMEM((24, LANES, LANES), F32),
                pltpu.VMEM((48, LANES, LANES), F32),
                pltpu.VMEM((24, 1056, LANES), F32),
                pltpu.VMEM((24, ROWS, LANES), F32),
                pltpu.VMEM((24, ROWS, LANES), F32),
                pltpu.VMEM((24, ROWS, LANES), F32),
                pltpu.VMEM((24, ROWS, LANES), F32),
                pltpu.VMEM((8, ROWS, LANES), F32),
                pltpu.VMEM((6, 2, 8, ROWS, LANES), F32),
                pltpu.VMEM((ROWS, 8, LANES), F32),
                pltpu.VMEM((9, 8, LANES), F32),
                pltpu.VMEM((4, 2, ROWS, LANES), F32),
                pltpu.VMEM((4, 2, ROWS, LANES), F32),
                dma((3, 3)), dma((3, 3)), dma((6, 2, 2)), dma((6, 2, 2)), dma((3,)), dma((3,)), dma((7,)), dma((7,)),
            ],
            compiler_params=pltpu.CompilerParams(collective_id=0, has_side_effects=True, vmem_limit_bytes=60 * BRICK * BRICK),
        )(u.reshape(BRICK, ROWS), f.reshape(BRICK, ROWS), kappa.reshape(BRICK, ROWS), w, om)
        out, rho = pl.pallas_call(
            unpack_kernel,
            out_shape=(jax.ShapeDtypeStruct((BRICK, ROWS), F32), jax.ShapeDtypeStruct((1, ROWS), F32)),
            in_specs=[vmem, vmem],
            out_specs=(vmem, vmem),
            compiler_params=pltpu.CompilerParams(vmem_limit_bytes=8 * BRICK * BRICK),
        )(dense, total)
        return out.reshape(ROWS, ROWS, ROWS), rho.reshape(ROWS)

    return jax.shard_map(local, mesh=mesh, in_specs=(field_spec, field_spec, field_spec, P(), P()),
                         out_specs=(field_spec, P('batch')), check_vma=False)
```

```python
import jax
import jax.numpy as jnp
from jax import lax
from jax.experimental import pallas as pl
from jax.experimental.pallas import tpu as pltpu
from jax.sharding import PartitionSpec as P

MESH = pl.DeviceIdType.MESH
F32 = jnp.float32
ROWS = 32
LANES = 128
MIB = 1024 * 1024
PITCH = 40
PITCHED = ROWS * PITCH
DEPTH = 8
BLOCKS = 4
CELLS = 64 * 64 * 64
OFFSETS = [(a, b, c) for a in (-1, 0, 1) for b in (-1, 0, 1) for c in (-1, 0, 1) if (a, b, c) != (0, 0, 0)]
TERM = {o: n for n, o in enumerate(OFFSETS)}


def rows_of(ref):
    return ref.reshape(ROWS, PITCH, ROWS).at[:, pl.ds(0, ROWS), :]


def kernel(u_ref, f_ref, k_ref, w_hbm, om_hbm, out_ref, rho_ref,
           w_ref, om_ref, bricks, brick_sem, pack, recv_own, kap, fld, coef, src_own, src_div, inv, diag, stage, halo, sums, psum, back, back_recv,
           own_send, own_recv, ring_send, ring_recv, back_send, back_recv_sem, sum_send, sum_recv):
    xc = lax.axis_index('x')
    yc = lax.axis_index('y')
    zc = lax.axis_index('z')
    me = 4 * zc + 2 * yc + xc
    turn = (yc + zc) % 2
    my_l = xc + 2 * turn
    my_q = 2 * xc + zc

    def slab_device(slab_y, slab_l):
        t = slab_l // 2
        return {'batch': 0, 'z': (slab_y + t) % 2, 'y': slab_y, 'x': slab_l % 2}

    def ring_device(step):
        s = (4 * yc + my_l + step + 8) % 8
        return slab_device(s // 4, s % 4)

    def device(i):
        return {'batch': 0, 'z': i // 4, 'y': (i // 2) % 2, 'x': i % 2}

    even = lax.broadcasted_iota(jnp.int32, (1, 8, LANES), 2) % 2 == 0
    top = lax.broadcasted_iota(jnp.int32, (1, 8, LANES), 1) == 0
    lane_in = lax.broadcasted_iota(jnp.int32, (LANES, LANES), 0)
    lane_out = lax.broadcasted_iota(jnp.int32, (LANES, LANES), 1)
    weave = (lane_out == 2 * (lane_in % 64) + lane_in // 64).astype(F32).astype(jnp.bfloat16)
    unweave = (lane_in == 2 * (lane_out % 64) + lane_out // 64).astype(F32).astype(jnp.bfloat16)

    def move_lanes(v, matrix):
        total = None
        for _ in range(3):
            part = v.astype(jnp.bfloat16)
            v = v - part.astype(F32)
            moved = jnp.dot(part, matrix, preferred_element_type=F32)
            total = moved if total is None else total + moved
        return total

    loads = [pltpu.make_async_copy(ref, rows_of(bricks.at[pl.ds(a * PITCHED, PITCHED)]), brick_sem.at[a]) for a, ref in enumerate((k_ref, u_ref, f_ref))]
    loads.append(pltpu.make_async_copy(w_hbm, w_ref, brick_sem.at[3]))
    loads.append(pltpu.make_async_copy(om_hbm, om_ref, brick_sem.at[4]))
    for load in loads:
        load.start()

    barrier = pltpu.get_barrier_semaphore()
    for r in range(1, 8):
        pl.semaphore_signal(barrier, inc=1, device_id=device((me + r) % 8), device_id_type=MESH)

    def pack_array(a):
        loads[a].wait()
        for i in range(8):
            rows = [bricks[pl.ds(a * PITCHED + 4 * i + m, ROWS, stride=PITCH), :] for m in range(4)]
            pack[a, i] = jnp.concatenate(rows, axis=1)

    def own_copy(a, r):
        dest = (my_l + r) % 4
        return pltpu.make_async_remote_copy(
            src_ref=pack.at[a, pl.ds(2 * dest, 2)], dst_ref=recv_own.at[a, my_q],
            send_sem=own_send.at[a, r - 1], recv_sem=own_recv.at[a, r - 1],
            device_id=slab_device(yc, dest), device_id_type=MESH)

    def send_own(a):
        for r in range(1, 4):
            own_copy(a, r).start()
        recv_own[a, my_q] = pack[a, pl.ds(2 * my_l, 2)]

    def row(ver, first):
        return slice(40 * ver + first, 40 * ver + first + ROWS)

    def put(dst, plane, v):
        dst[pl.ds(plane, v.shape[0]), row(1, 8), :] = v
        put_turned(dst, plane, v)

    def put_turned(dst, plane, v):
        planes = pl.ds(plane, v.shape[0])
        dst[planes, row(0, 8), :] = pltpu.roll(v, 2, 2)
        dst[planes, row(2, 8), :] = pltpu.roll(v, 126, 2)
        edge = jnp.where(top, v[:, 0:8], v[:, 24:ROWS])
        r1, r3, r125, r127 = (pltpu.roll(edge, s, 2) for s in (1, 3, 125, 127))
        for ver, a, b in ((0, r1, r3), (1, r127, r1), (2, r125, r127)):
            swap = jnp.where(even, a, b)
            dst[planes, 40 * ver + 7:40 * ver + 8, :] = swap[:, 7:8]
            dst[planes, 40 * ver + 40:40 * ver + 41, :] = swap[:, 0:1]

    def wait_own(a):
        for r in range(1, 4):
            own_copy(a, r).wait_recv()

    def unpack_own(a, store):
        planes = [jnp.concatenate([recv_own[a, q, yy, :, ROWS * m:ROWS * m + ROWS] for q in range(4)], axis=1)
                  for yy in range(2) for m in range(4)]
        store(move_lanes(jnp.concatenate(planes, axis=0), weave).reshape(8, ROWS, LANES))

    def ring_copy(e, src, dst, side, part):
        first = 4 * (1 - part) if side == 0 else 4 * part
        return pltpu.make_async_remote_copy(
            src_ref=src(first), dst_ref=dst(side, first),
            send_sem=ring_send.at[e, side, part], recv_sem=ring_recv.at[e, side, part],
            device_id=ring_device(1 if side == 0 else -1), device_id_type=MESH)

    def halo_dst(e):
        return lambda side, first: halo.at[e, side, pl.ds(first, 4)]

    def kap_copy(side, part):
        return ring_copy(0, lambda first: kap.at[pl.ds(8 + first, 4), pl.ds(48, ROWS), :], halo_dst(0), side, part)

    def f_copy(side, part):
        return ring_copy(1, lambda first: src_own.at[pl.ds(8 + first, 4)],
                         lambda side, first: src_own.at[pl.ds(16 * side + first, 4)], side, part)

    def u_copy(e, side, part):
        return ring_copy(e, lambda first: stage.at[pl.ds(first, 4)], halo_dst(e), side, part)

    PARTS = [(side, part) for part in range(2) for side in range(2)]

    def unpack_halo(e, dst, part):
        for side in range(2):
            j = 4 * (1 - part) if side == 0 else 4 * part
            put(dst, 16 * side + j, halo[e, side, j:j + 4])

    pack_array(0)
    pl.semaphore_wait(barrier, 7)
    send_own(0)
    pack_array(1)
    send_own(1)
    pack_array(2)
    send_own(2)

    wait_own(0)
    unpack_own(0, lambda v: put(kap, 8, v))
    for side in range(2):
        kap_copy(side, 0).start()
    wait_own(1)

    def store_u(v):
        stage[...] = v
        put(fld, 8, v)
    unpack_own(1, store_u)
    for side in range(2):
        u_copy(2, side, 0).start()
    for side in range(2):
        kap_copy(side, 1).start()
    wait_own(2)

    def store_f(v):
        src_own[8:16] = v
    unpack_own(2, store_f)
    for side in range(2):
        f_copy(side, 0).start()
    for side in range(2):
        u_copy(2, side, 1).start()
    for side in range(2):
        f_copy(side, 1).start()

    loads[3].wait()
    loads[4].wait()
    half_w = [0.5 * w_ref[n] for n in range(26)]

    def coef_plane(p, _):
        for g in range(4):
            rows = pl.ds(8 * g, 8)
            center = kap[p, 48 + 8 * g:56 + 8 * g, :]
            terms = []
            total = None
            for n, (ox, oy, oz) in enumerate(OFFSETS):
                first = 40 * (oz + 1) + 8 + 8 * g + ox
                near = kap[p + oy, first:first + 8, :]
                c = half_w[n] * (center + near)
                terms.append(c)
                total = c if total is None else total + c
            recip = 1.0 / total
            inv[p, rows, :] = recip
            diag[p, rows, :] = jnp.where(jnp.logical_and(p >= 8, p < 16), total, 0.0)
            for n in range(26):
                coef[p, 40 * n + 8 * g:40 * n + 8 * g + 8, :] = terms[n] * recip
        return 0
    def scale_f(p, _):
        src_div[p] = src_own[p] * inv[p]
        return 0

    def coef_range(lo, hi):
        lax.fori_loop(lo, hi, coef_plane, 0)

    def scale_range(lo, hi):
        lax.fori_loop(lo, hi, scale_f, 0)

    sums[...] = jnp.zeros_like(sums)
    coef_range(9, 15)
    scale_range(9, 15)
    for part in range(2):
        for side in range(2):
            kap_copy(side, part).wait()
        unpack_halo(0, kap, part)
        coef_range(*((5, 9) if part == 0 else (1, 5)))
        coef_range(*((15, 19) if part == 0 else (19, 23)))

    def pair(level, first, second, n, before, blk):
        src, dst = (0, 24) if level % 2 == 1 else (24, 0)
        k = DEPTH * blk + level - 1
        om = om_ref[k]
        owned = first + n > 8

        def body(s, _):
            lo = first + s * (second - first)
            last = before + s * (dst + first - before)
            turned = fld[pl.ds(last, 4), row(1, 8), :]
            center = fld[pl.ds(src + lo, n), row(1, 8), :]
            acc = src_div[pl.ds(lo, n)] - center
            for ox in (-1, 0, 1):
                for oz in (-1, 0, 1):
                    near = fld[pl.ds(src + lo - 1, n + 2), row(oz + 1, 8 + ox), :]
                    for oy in (-1, 0, 1):
                        if (ox, oy, oz) != (0, 0, 0):
                            t = 40 * TERM[(ox, oy, oz)]
                            acc = acc + coef[pl.ds(lo, n), t:t + ROWS, :] * near[1 + oy:1 + oy + n]
            new = center + om * acc
            fld[pl.ds(dst + lo, n), row(1, 8), :] = new
            put_turned(fld, last, turned)
            if level == DEPTH:
                stage[pl.ds(lo - 8, n)] = new
            if owned:
                r = acc * diag[pl.ds(lo, n)]
                r = jnp.sum(r * r, axis=0)
                sums[k] = sums[k] + ((r[0:8] + r[8:16]) + (r[16:24] + r[24:ROWS]))
            return 0
        if first == second:
            body(0, 0)
        else:
            lax.fori_loop(0, 2, body, 0)
        return dst + second

    def flush(before):
        put_turned(fld, before, fld[pl.ds(before, 4), row(1, 8), :])
        return before

    def block(blk, _):
        e = 2 + blk
        before = 8
        for level, first, second, n in ((1, 9, 12, 3), (2, 10, 10, 4), (3, 11, 11, 2)):
            before = flush(pair(level, first, second, n, before, blk))
        for part in range(2):
            @pl.when(blk == 0)
            def _():
                left, right = (5, 15) if part == 0 else (1, 19)
                for side in range(2):
                    f_copy(side, part).wait()
                scale_range(left, left + 4)
                scale_range(right, right + 4)
            for side in range(2):
                u_copy(e, side, part).wait()
            unpack_halo(e, fld, part)
            if part == 0:
                for level in range(1, 4):
                    before = pair(level, 4 + level, 16 - level, 4, before, blk)
            else:
                for level in range(1, 9):
                    before = pair(level, level, 20 - level, 4, before, blk)
                    if level < 5:
                        first, second, n = ((8, 12, 4), (9, 12, 3), (10, 10, 4), (11, 11, 2))[level - 1]
                        before = pair(3 + level, first, second, n, before, blk)

        @pl.when(blk < BLOCKS - 1)
        def _():
            for side, part in PARTS:
                u_copy(e + 1, side, part).start()
            flush(before)
        return 0
    lax.fori_loop(0, BLOCKS, block, 0)

    def sum_copy(r):
        return pltpu.make_async_remote_copy(
            src_ref=psum.at[8], dst_ref=psum.at[me], send_sem=sum_send.at[r - 1], recv_sem=sum_recv.at[r - 1],
            device_id=device((me + r) % 8), device_id_type=MESH)

    def back_copy(r):
        q = (my_q + r) % 4
        return pltpu.make_async_remote_copy(
            src_ref=back.at[q], dst_ref=back_recv.at[my_l], send_sem=back_send.at[r - 1], recv_sem=back_recv_sem.at[r - 1],
            device_id={'batch': 0, 'z': q % 2, 'y': yc, 'x': q // 2}, device_id_type=MESH)

    planes8 = move_lanes(stage[...].reshape(8 * ROWS, LANES), unweave).reshape(8, ROWS, LANES)
    for yy in range(2):
        planes = [planes8[4 * yy + m] for m in range(4)]
        for q in range(4):
            back[q, yy] = jnp.concatenate([v[:, ROWS * q:ROWS * q + ROWS] for v in planes], axis=1)
    for r in range(1, 4):
        back_copy(r).start()
    back_recv[my_l] = back[my_q]
    flat = jnp.sum(sums[...], axis=1)
    flat = jnp.concatenate([flat, jnp.zeros((96, LANES), F32)], axis=0)
    mine = jnp.sum(flat.T, axis=0, keepdims=True)
    mine = jnp.broadcast_to(mine, (8, LANES))
    psum[8] = mine
    psum[me] = mine
    for r in range(1, 8):
        sum_copy(r).start()

    for r in range(1, 4):
        back_copy(r).wait()
    out_ref[...] = back_recv[...]
    for r in range(1, 8):
        sum_copy(r).wait()
    total = psum[0]
    for i in range(1, 8):
        total = total + psum[i]
    rho_ref[...] = total

    for a in range(3):
        for r in range(1, 4):
            own_copy(a, r).wait_send()


def unpack_kernel(dense_ref, total_ref, out_ref, rho_ref):
    for i in range(8):
        v = dense_ref[i // 2, i % 2]
        for m in range(4):
            out_ref[pl.ds(4 * i + m, ROWS, stride=ROWS), :] = v[:, ROWS * m:ROWS * m + ROWS]
    rho_ref[...] = jnp.sqrt(total_ref[...] / CELLS)[0:1, 0:ROWS]


def solution(mesh):
    field_spec = P(('batch', 'x'), 'y', 'z')

    def local(u, f, kappa, w, om):
        vmem = pl.BlockSpec(memory_space=pltpu.VMEM)
        hbm = pl.BlockSpec(memory_space=pltpu.HBM)
        dma = pltpu.SemaphoreType.DMA
        dense, total = pl.pallas_call(
            kernel,
            out_shape=(pltpu.VMEM((4, 2, ROWS, LANES), F32), pltpu.VMEM((8, LANES), F32)),
            in_specs=[hbm] * 5,
            out_specs=(vmem, vmem),
            scratch_shapes=[
                pltpu.SMEM((26,), F32),
                pltpu.SMEM((ROWS,), F32),
                pltpu.VMEM((3 * PITCHED, ROWS), F32),
                dma((5,)),
                pltpu.VMEM((3, 8, ROWS, LANES), F32),
                pltpu.VMEM((3, 4, 2, ROWS, LANES), F32),
                pltpu.VMEM((24, LANES, LANES), F32),
                pltpu.VMEM((48, LANES, LANES), F32),
                pltpu.VMEM((24, 1056, LANES), F32),
                pltpu.VMEM((24, ROWS, LANES), F32),
                pltpu.VMEM((24, ROWS, LANES), F32),
                pltpu.VMEM((24, ROWS, LANES), F32),
                pltpu.VMEM((24, ROWS, LANES), F32),
                pltpu.VMEM((8, ROWS, LANES), F32),
                pltpu.VMEM((6, 2, 8, ROWS, LANES), F32),
                pltpu.VMEM((ROWS, 8, LANES), F32),
                pltpu.VMEM((9, 8, LANES), F32),
                pltpu.VMEM((4, 2, ROWS, LANES), F32),
                pltpu.VMEM((4, 2, ROWS, LANES), F32),
                dma((3, 3)), dma((3, 3)), dma((6, 2, 2)), dma((6, 2, 2)), dma((3,)), dma((3,)), dma((7,)), dma((7,)),
            ],
            compiler_params=pltpu.CompilerParams(collective_id=0, has_side_effects=True, vmem_limit_bytes=60 * MIB),
        )(u, f, kappa, w, om)
        out, rho = pl.pallas_call(
            unpack_kernel,
            out_shape=(jax.ShapeDtypeStruct((ROWS * ROWS, ROWS), F32), jax.ShapeDtypeStruct((1, ROWS), F32)),
            in_specs=[vmem, vmem],
            out_specs=(vmem, vmem),
            compiler_params=pltpu.CompilerParams(vmem_limit_bytes=8 * MIB),
        )(dense, total)
        return out.reshape(ROWS, ROWS, ROWS), rho.reshape(ROWS)

    return jax.shard_map(local, mesh=mesh, in_specs=(field_spec, field_spec, field_spec, P(), P()),
                         out_specs=(field_spec, P('batch')), check_vma=False)
```

```python
import jax
import jax.numpy as jnp
from jax import lax
from jax.experimental import pallas as pl
from jax.experimental.pallas import tpu as pltpu
from jax.sharding import PartitionSpec as P

MESH = pl.DeviceIdType.MESH
F32 = jnp.float32
ROWS = 32
LANES = 128
MIB = 1024 * 1024
PITCH = 40
PITCHED = ROWS * PITCH
DEPTH = 8
BLOCKS = 4
CELLS = 64 * 64 * 64
OFFSETS = [(a, b, c) for a in (-1, 0, 1) for b in (-1, 0, 1) for c in (-1, 0, 1) if (a, b, c) != (0, 0, 0)]
TERM = {o: n for n, o in enumerate(OFFSETS)}


def rows_of(ref):
    return ref.reshape(ROWS, PITCH, ROWS).at[:, pl.ds(0, ROWS), :]


def kernel(u_ref, f_ref, k_ref, w_hbm, om_hbm, out_ref, rho_ref,
           w_ref, om_ref, bricks, brick_sem, pack, recv_own, kap, fld, coef, src_own, src_div, inv, diag, stage, halo, sums, psum, back, back_recv,
           own_send, own_recv, ring_send, ring_recv, back_send, back_recv_sem, sum_send, sum_recv):
    xc = lax.axis_index('x')
    yc = lax.axis_index('y')
    zc = lax.axis_index('z')
    me = 4 * zc + 2 * yc + xc
    turn = (yc + zc) % 2
    my_l = xc + 2 * turn
    my_q = 2 * xc + zc

    def slab_device(slab_y, slab_l):
        t = slab_l // 2
        return {'batch': 0, 'z': (slab_y + t) % 2, 'y': slab_y, 'x': slab_l % 2}

    def ring_device(step):
        s = (4 * yc + my_l + step + 8) % 8
        return slab_device(s // 4, s % 4)

    def device(i):
        return {'batch': 0, 'z': i // 4, 'y': (i // 2) % 2, 'x': i % 2}

    even = lax.broadcasted_iota(jnp.int32, (1, 8, LANES), 2) % 2 == 0
    top = lax.broadcasted_iota(jnp.int32, (1, 8, LANES), 1) == 0
    lane_in = lax.broadcasted_iota(jnp.int32, (LANES, LANES), 0)
    lane_out = lax.broadcasted_iota(jnp.int32, (LANES, LANES), 1)
    weave = (lane_out == 2 * (lane_in % 64) + lane_in // 64).astype(F32).astype(jnp.bfloat16)
    unweave = (lane_in == 2 * (lane_out % 64) + lane_out // 64).astype(F32).astype(jnp.bfloat16)

    def move_lanes(v, matrix):
        total = None
        for _ in range(3):
            part = v.astype(jnp.bfloat16)
            v = v - part.astype(F32)
            moved = jnp.dot(part, matrix, preferred_element_type=F32)
            total = moved if total is None else total + moved
        return total

    loads = [pltpu.make_async_copy(ref, rows_of(bricks.at[pl.ds(a * PITCHED, PITCHED)]), brick_sem.at[a]) for a, ref in enumerate((k_ref, u_ref, f_ref))]
    loads.append(pltpu.make_async_copy(w_hbm, w_ref, brick_sem.at[3]))
    loads.append(pltpu.make_async_copy(om_hbm, om_ref, brick_sem.at[4]))
    for load in loads:
        load.start()

    barrier = pltpu.get_barrier_semaphore()
    for r in range(1, 8):
        pl.semaphore_signal(barrier, inc=1, device_id=device((me + r) % 8), device_id_type=MESH)

    def pack_array(a):
        loads[a].wait()
        for i in range(8):
            rows = [bricks[pl.ds(a * PITCHED + 4 * i + m, ROWS, stride=PITCH), :] for m in range(4)]
            pack[a, i] = jnp.concatenate(rows, axis=1)

    def own_copy(a, r):
        dest = (my_l + r) % 4
        return pltpu.make_async_remote_copy(
            src_ref=pack.at[a, pl.ds(2 * dest, 2)], dst_ref=recv_own.at[a, my_q],
            send_sem=own_send.at[a, r - 1], recv_sem=own_recv.at[a, r - 1],
            device_id=slab_device(yc, dest), device_id_type=MESH)

    def send_own(a):
        for r in range(1, 4):
            own_copy(a, r).start()
        recv_own[a, my_q] = pack[a, pl.ds(2 * my_l, 2)]

    def row(ver, first):
        return slice(40 * ver + first, 40 * ver + first + ROWS)

    def put(dst, plane, v):
        dst[pl.ds(plane, v.shape[0]), row(1, 8), :] = v
        put_turned(dst, plane, v)

    def put_turned(dst, plane, v):
        planes = pl.ds(plane, v.shape[0])
        dst[planes, row(0, 8), :] = pltpu.roll(v, 2, 2)
        dst[planes, row(2, 8), :] = pltpu.roll(v, 126, 2)
        edge = jnp.where(top, v[:, 0:8], v[:, 24:ROWS])
        r1, r3, r125, r127 = (pltpu.roll(edge, s, 2) for s in (1, 3, 125, 127))
        for ver, a, b in ((0, r1, r3), (1, r127, r1), (2, r125, r127)):
            swap = jnp.where(even, a, b)
            dst[planes, 40 * ver + 7:40 * ver + 8, :] = swap[:, 7:8]
            dst[planes, 40 * ver + 40:40 * ver + 41, :] = swap[:, 0:1]

    def wait_own(a):
        for r in range(1, 4):
            own_copy(a, r).wait_recv()

    def unpack_own(a, store):
        planes = [jnp.concatenate([recv_own[a, q, yy, :, ROWS * m:ROWS * m + ROWS] for q in range(4)], axis=1)
                  for yy in range(2) for m in range(4)]
        store(move_lanes(jnp.concatenate(planes, axis=0), weave).reshape(8, ROWS, LANES))

    def part_start(side, part):
        return 4 * (1 - part) * (1 - side) + 4 * part * side

    def ring_copy(e, src, dst, side, part):
        first = part_start(side, part)
        return pltpu.make_async_remote_copy(
            src_ref=src(first), dst_ref=dst(side, first),
            send_sem=ring_send.at[e, side, part], recv_sem=ring_recv.at[e, side, part],
            device_id=ring_device(1 - 2 * side), device_id_type=MESH)

    def halo_dst(e):
        return lambda side, first: halo.at[e, side, pl.ds(first, 4)]

    def kap_copy(side, part):
        return ring_copy(0, lambda first: kap.at[pl.ds(8 + first, 4), pl.ds(48, ROWS), :], halo_dst(0), side, part)

    def f_copy(side, part):
        return ring_copy(1, lambda first: src_own.at[pl.ds(8 + first, 4)],
                         lambda side, first: src_own.at[pl.ds(16 * side + first, 4)], side, part)

    def u_copy(e, side, part):
        return ring_copy(e, lambda first: stage.at[pl.ds(first, 4)], halo_dst(e), side, part)

    PARTS = [(side, part) for part in range(2) for side in range(2)]

    def unpack_side(e, dst, side, part):
        j = part_start(side, part)
        put(dst, 16 * side + j, halo[e, side, pl.ds(j, 4)])

    pack_array(0)
    pl.semaphore_wait(barrier, 7)
    send_own(0)
    pack_array(1)
    send_own(1)
    pack_array(2)
    send_own(2)

    wait_own(0)
    unpack_own(0, lambda v: put(kap, 8, v))
    for side in range(2):
        kap_copy(side, 0).start()
    wait_own(1)

    def store_u(v):
        stage[...] = v
        put(fld, 8, v)
    unpack_own(1, store_u)
    for side in range(2):
        u_copy(2, side, 0).start()
    for side in range(2):
        kap_copy(side, 1).start()
    wait_own(2)

    def store_f(v):
        src_own[8:16] = v
    unpack_own(2, store_f)
    for side in range(2):
        f_copy(side, 0).start()
    for side in range(2):
        u_copy(2, side, 1).start()
    for side in range(2):
        f_copy(side, 1).start()

    loads[3].wait()
    loads[4].wait()
    half_w = [0.5 * w_ref[n] for n in range(26)]

    def coef_plane(p, _):
        for g in range(4):
            rows = pl.ds(8 * g, 8)
            center = kap[p, 48 + 8 * g:56 + 8 * g, :]
            terms = []
            total = None
            for n, (ox, oy, oz) in enumerate(OFFSETS):
                first = 40 * (oz + 1) + 8 + 8 * g + ox
                near = kap[p + oy, first:first + 8, :]
                c = half_w[n] * (center + near)
                terms.append(c)
                total = c if total is None else total + c
            recip = 1.0 / total
            inv[p, rows, :] = recip
            diag[p, rows, :] = jnp.where(jnp.logical_and(p >= 8, p < 16), total, 0.0)
            for n in range(26):
                coef[p, 40 * n + 8 * g:40 * n + 8 * g + 8, :] = terms[n] * recip
        return 0
    def scale_f(p, _):
        src_div[p] = src_own[p] * inv[p]
        return 0

    def coef_range(lo, hi):
        lax.fori_loop(lo, hi, coef_plane, 0)

    def scale_range(lo, hi):
        lax.fori_loop(lo, hi, scale_f, 0)

    sums[...] = jnp.zeros_like(sums)
    coef_range(9, 15)
    scale_range(9, 15)
    for part in range(2):
        for side in range(2):
            kap_copy(side, part).wait()
            unpack_side(0, kap, side, part)
        coef_range(*((5, 9) if part == 0 else (1, 5)))
        coef_range(*((15, 19) if part == 0 else (19, 23)))
    scale_range(8, 9)
    scale_range(15, 16)

    def strip(level, left, n, right, before, blk, final=False):
        src = 24 * ((level + 1) % 2)
        dst = 24 - src
        lo = left + right * (24 - n - 2 * left)
        k = DEPTH * blk + level - 1
        turned = fld[pl.ds(before, 4), row(1, 8), :]
        center = fld[pl.ds(src + lo, n), row(1, 8), :]
        acc = src_div[pl.ds(lo, n)] - center
        for ox in (-1, 0, 1):
            for oz in (-1, 0, 1):
                near = fld[pl.ds(src + lo - 1, n + 2), row(oz + 1, 8 + ox), :]
                for oy in (-1, 0, 1):
                    if (ox, oy, oz) != (0, 0, 0):
                        t = 40 * TERM[(ox, oy, oz)]
                        acc = acc + coef[pl.ds(lo, n), t:t + ROWS, :] * near[1 + oy:1 + oy + n]
        new = center + om_ref[k] * acc
        fld[pl.ds(dst + lo, n), row(1, 8), :] = new
        put_turned(fld, before, turned)
        if final:
            stage[pl.ds(lo - 8, n)] = new
        r = acc * diag[pl.ds(lo, n)]
        r = jnp.sum(r * r, axis=0)
        sums[k] = sums[k] + ((r[0:8] + r[8:16]) + (r[16:24] + r[24:32]))
        return dst + lo

    def flush(before):
        put_turned(fld, before, fld[pl.ds(before, 4), row(1, 8), :])
        return before

    fast = 1 - xc
    slow = xc

    def fast_pass(t, before, blk):
        level = 1 + t // 2
        return strip(level, level + 4 * (1 - t % 2), 4, fast, before, blk)

    def block(blk, _):
        e = 2 + blk
        before = strip(1, 9, 3, 0, 8, blk)
        before = flush(strip(1, 9, 3, 1, before, blk))
        before = flush(strip(2, 10, 4, 0, before, blk))
        before = flush(strip(3, 11, 2, 0, before, blk))

        @pl.when(blk == 0)
        def _():
            for part in range(2):
                f_copy(fast, part).wait_recv()
            scale_range(1 + 15 * fast, 8 + 15 * fast)
        for part in range(2):
            u_copy(e, fast, part).wait_recv()
        for part in range(2):
            unpack_side(e, fld, fast, part)
        before = lax.fori_loop(0, 8, lambda t, b: fast_pass(t, b, blk), before)

        @pl.when(blk == 0)
        def _():
            f_copy(slow, 0).wait_recv()
            scale_range(4 + 12 * slow, 8 + 12 * slow)
        u_copy(e, slow, 0).wait_recv()
        unpack_side(e, fld, slow, 0)
        before = lax.fori_loop(0, 2, lambda s, b: strip(1 + 4 * s, 5, 4, slow + s * (fast - slow), b, blk), before)
        before = flush(strip(2, 6, 4, slow, before, blk))
        before = strip(3, 7, 4, slow, before, blk)

        @pl.when(blk == 0)
        def _():
            f_copy(slow, 1).wait_recv()
            scale_range(1 + 19 * slow, 4 + 19 * slow)
            for side, part in PARTS:
                f_copy(side, part).wait_send()
        u_copy(e, slow, 1).wait_recv()
        for side, part in PARTS:
            u_copy(e, side, part).wait_send()
        unpack_side(e, fld, slow, 1)
        before = lax.fori_loop(0, 2, lambda s, b: strip(1 + 3 * s, 1 + 7 * s, 4, slow, b, blk), before)
        before = strip(2, 2, 4, slow, before, blk)
        before = lax.fori_loop(0, 2, lambda s, b: strip(5, 9, 3, s, b, blk), before)
        before = lax.fori_loop(0, 2, lambda s, b: strip(3 + 3 * s, 3 + 7 * s, 4, slow, b, blk), before)
        before = strip(4, 4, 4, slow, before, blk)
        before = strip(7, 11, 2, 0, before, blk)
        before = strip(5, 5, 4, slow, before, blk)
        before = lax.fori_loop(
            0, 4, lambda t, b: strip(6 + t // 2, 6 + t // 2, 4, fast + (t % 2) * (slow - fast), b, blk), before)
        before = lax.fori_loop(0, 2, lambda s, b: strip(8, 8, 4, fast + s * (slow - fast), b, blk, True), before)

        @pl.when(blk < BLOCKS - 1)
        def _():
            for side, part in PARTS:
                u_copy(e + 1, side, part).start()
            flush(before)
        return 0
    lax.fori_loop(0, BLOCKS, block, 0)

    def sum_copy(r):
        return pltpu.make_async_remote_copy(
            src_ref=psum.at[8], dst_ref=psum.at[me], send_sem=sum_send.at[r - 1], recv_sem=sum_recv.at[r - 1],
            device_id=device((me + r) % 8), device_id_type=MESH)

    def back_copy(r):
        q = (my_q + r) % 4
        return pltpu.make_async_remote_copy(
            src_ref=back.at[q], dst_ref=back_recv.at[my_l], send_sem=back_send.at[r - 1], recv_sem=back_recv_sem.at[r - 1],
            device_id={'batch': 0, 'z': q % 2, 'y': yc, 'x': q // 2}, device_id_type=MESH)

    planes8 = move_lanes(stage[...].reshape(8 * ROWS, LANES), unweave).reshape(8, ROWS, LANES)
    for yy in range(2):
        planes = [planes8[4 * yy + m] for m in range(4)]
        for q in range(4):
            back[q, yy] = jnp.concatenate([v[:, ROWS * q:ROWS * q + ROWS] for v in planes], axis=1)
    for r in range(1, 4):
        back_copy(r).start()
    back_recv[my_l] = back[my_q]
    flat = jnp.sum(sums[...], axis=1)
    flat = jnp.concatenate([flat, jnp.zeros((96, LANES), F32)], axis=0)
    mine = jnp.sum(flat.T, axis=0, keepdims=True)
    mine = jnp.broadcast_to(mine, (8, LANES))
    psum[8] = mine
    psum[me] = mine
    for r in range(1, 8):
        sum_copy(r).start()

    for r in range(1, 4):
        back_copy(r).wait()
    out_ref[...] = back_recv[...]
    for r in range(1, 8):
        sum_copy(r).wait()
    total = psum[0]
    for i in range(1, 8):
        total = total + psum[i]
    rho_ref[...] = total

    for a in range(3):
        for r in range(1, 4):
            own_copy(a, r).wait_send()


def unpack_kernel(dense_ref, total_ref, out_ref, rho_ref):
    for i in range(8):
        v = dense_ref[i // 2, i % 2]
        for m in range(4):
            out_ref[pl.ds(4 * i + m, ROWS, stride=ROWS), :] = v[:, ROWS * m:ROWS * m + ROWS]
    rho_ref[...] = jnp.sqrt(total_ref[...] / CELLS)[0:1, 0:ROWS]


def solution(mesh):
    field_spec = P(('batch', 'x'), 'y', 'z')

    def local(u, f, kappa, w, om):
        vmem = pl.BlockSpec(memory_space=pltpu.VMEM)
        hbm = pl.BlockSpec(memory_space=pltpu.HBM)
        dma = pltpu.SemaphoreType.DMA
        dense, total = pl.pallas_call(
            kernel,
            out_shape=(pltpu.VMEM((4, 2, ROWS, LANES), F32), pltpu.VMEM((8, LANES), F32)),
            in_specs=[hbm] * 5,
            out_specs=(vmem, vmem),
            scratch_shapes=[
                pltpu.SMEM((26,), F32),
                pltpu.SMEM((ROWS,), F32),
                pltpu.VMEM((3 * PITCHED, ROWS), F32),
                dma((5,)),
                pltpu.VMEM((3, 8, ROWS, LANES), F32),
                pltpu.VMEM((3, 4, 2, ROWS, LANES), F32),
                pltpu.VMEM((24, LANES, LANES), F32),
                pltpu.VMEM((48, LANES, LANES), F32),
                pltpu.VMEM((24, 1056, LANES), F32),
                pltpu.VMEM((24, ROWS, LANES), F32),
                pltpu.VMEM((24, ROWS, LANES), F32),
                pltpu.VMEM((24, ROWS, LANES), F32),
                pltpu.VMEM((24, ROWS, LANES), F32),
                pltpu.VMEM((8, ROWS, LANES), F32),
                pltpu.VMEM((6, 2, 8, ROWS, LANES), F32),
                pltpu.VMEM((ROWS, 8, LANES), F32),
                pltpu.VMEM((9, 8, LANES), F32),
                pltpu.VMEM((4, 2, ROWS, LANES), F32),
                pltpu.VMEM((4, 2, ROWS, LANES), F32),
                dma((3, 3)), dma((3, 3)), dma((6, 2, 2)), dma((6, 2, 2)), dma((3,)), dma((3,)), dma((7,)), dma((7,)),
            ],
            compiler_params=pltpu.CompilerParams(collective_id=0, has_side_effects=True, vmem_limit_bytes=60 * MIB),
        )(u, f, kappa, w, om)
        out, rho = pl.pallas_call(
            unpack_kernel,
            out_shape=(jax.ShapeDtypeStruct((ROWS * ROWS, ROWS), F32), jax.ShapeDtypeStruct((1, ROWS), F32)),
            in_specs=[vmem, vmem],
            out_specs=(vmem, vmem),
            compiler_params=pltpu.CompilerParams(vmem_limit_bytes=8 * MIB),
        )(dense, total)
        return out.reshape(ROWS, ROWS, ROWS), rho.reshape(ROWS)

    return jax.shard_map(local, mesh=mesh, in_specs=(field_spec, field_spec, field_spec, P(), P()),
                         out_specs=(field_spec, P('batch')), check_vma=False)
```

```python
import jax
import jax.numpy as jnp
from jax import lax
from jax.experimental import pallas as pl
from jax.experimental.pallas import tpu as pltpu
from jax.sharding import PartitionSpec as P

MESH = pl.DeviceIdType.MESH
F32 = jnp.float32
ROWS = 32
LANES = 128
MIB = 1024 * 1024
PITCH = 40
PITCHED = ROWS * PITCH
DEPTH = 8
BLOCKS = 4
CELLS = 64 * 64 * 64
OFFSETS = [(a, b, c) for a in (-1, 0, 1) for b in (-1, 0, 1) for c in (-1, 0, 1) if (a, b, c) != (0, 0, 0)]
TERM = {o: n for n, o in enumerate(OFFSETS)}


def rows_of(ref):
    return ref.reshape(ROWS, PITCH, ROWS).at[:, pl.ds(0, ROWS), :]


def kernel(u_ref, f_ref, k_ref, w_hbm, om_hbm, out_ref, rho_ref,
           w_ref, om_ref, bricks, brick_sem, pack, recv_own, kap, fld, coef, src_own, src_div, inv, diag, stage, halo, sums, psum, back, back_recv,
           own_send, own_recv, ring_send, ring_recv, back_send, back_recv_sem, sum_send, sum_recv):
    xc = lax.axis_index('x')
    yc = lax.axis_index('y')
    zc = lax.axis_index('z')
    me = 4 * zc + 2 * yc + xc
    turn = (yc + zc) % 2
    my_l = xc + 2 * turn
    my_q = 2 * xc + zc

    fast = 1 - xc
    slow = xc

    def slab_device(slab_y, slab_l):
        t = slab_l // 2
        return {'batch': 0, 'z': (slab_y + t) % 2, 'y': slab_y, 'x': slab_l % 2}

    def ring_device(step):
        s = (4 * yc + my_l + step + 8) % 8
        return slab_device(s // 4, s % 4)

    def device(i):
        return {'batch': 0, 'z': i // 4, 'y': (i // 2) % 2, 'x': i % 2}

    even = lax.broadcasted_iota(jnp.int32, (1, 8, LANES), 2) % 2 == 0
    top = lax.broadcasted_iota(jnp.int32, (1, 8, LANES), 1) == 0
    lane_in = lax.broadcasted_iota(jnp.int32, (LANES, LANES), 0)
    lane_out = lax.broadcasted_iota(jnp.int32, (LANES, LANES), 1)
    weave = (lane_out == 2 * (lane_in % 64) + lane_in // 64).astype(F32).astype(jnp.bfloat16)
    unweave = (lane_in == 2 * (lane_out % 64) + lane_out // 64).astype(F32).astype(jnp.bfloat16)

    def move_lanes(v, matrix):
        total = None
        for _ in range(3):
            part = v.astype(jnp.bfloat16)
            v = v - part.astype(F32)
            moved = jnp.dot(part, matrix, preferred_element_type=F32)
            total = moved if total is None else total + moved
        return total

    loads = [pltpu.make_async_copy(ref, rows_of(bricks.at[pl.ds(a * PITCHED, PITCHED)]), brick_sem.at[a]) for a, ref in enumerate((k_ref, u_ref, f_ref))]
    loads.append(pltpu.make_async_copy(w_hbm, w_ref, brick_sem.at[3]))
    loads.append(pltpu.make_async_copy(om_hbm, om_ref, brick_sem.at[4]))
    for load in loads:
        load.start()

    barrier = pltpu.get_barrier_semaphore()
    for r in range(1, 8):
        pl.semaphore_signal(barrier, inc=1, device_id=device((me + r) % 8), device_id_type=MESH)

    def pack_array(a):
        loads[a].wait()
        for i in range(8):
            rows = [bricks[pl.ds(a * PITCHED + 4 * i + m, ROWS, stride=PITCH), :] for m in range(4)]
            pack[a, i] = jnp.concatenate(rows, axis=1)

    def own_copy(a, r):
        dest = (my_l + r) % 4
        return pltpu.make_async_remote_copy(
            src_ref=pack.at[a, pl.ds(2 * dest, 2)], dst_ref=recv_own.at[a, my_q],
            send_sem=own_send.at[a, r - 1], recv_sem=own_recv.at[a, r - 1],
            device_id=slab_device(yc, dest), device_id_type=MESH)

    def send_own(a):
        for r in range(1, 4):
            own_copy(a, r).start()
        recv_own[a, my_q] = pack[a, pl.ds(2 * my_l, 2)]

    def row(ver, first):
        return slice(40 * ver + first, 40 * ver + first + ROWS)

    def put(dst, plane, v):
        dst[pl.ds(plane, v.shape[0]), row(1, 8), :] = v
        put_turned(dst, plane, v)

    def put_turned(dst, plane, v):
        planes = pl.ds(plane, v.shape[0])
        dst[planes, row(0, 8), :] = pltpu.roll(v, 2, 2)
        dst[planes, row(2, 8), :] = pltpu.roll(v, 126, 2)
        edge = jnp.where(top, v[:, 0:8], v[:, 24:ROWS])
        r1, r3, r125, r127 = (pltpu.roll(edge, s, 2) for s in (1, 3, 125, 127))
        for ver, a, b in ((0, r1, r3), (1, r127, r1), (2, r125, r127)):
            swap = jnp.where(even, a, b)
            dst[planes, 40 * ver + 7:40 * ver + 8, :] = swap[:, 7:8]
            dst[planes, 40 * ver + 40:40 * ver + 41, :] = swap[:, 0:1]

    def wait_own(a):
        for r in range(1, 4):
            own_copy(a, r).wait_recv()

    def unpack_own(a, store):
        planes = [jnp.concatenate([recv_own[a, q, yy, :, ROWS * m:ROWS * m + ROWS] for q in range(4)], axis=1)
                  for yy in range(2) for m in range(4)]
        store(move_lanes(jnp.concatenate(planes, axis=0), weave).reshape(8, ROWS, LANES))

    def part_start(side, part):
        return 4 * (1 - part) * (1 - side) + 4 * part * side

    def ring_copy(e, src, dst, side, part):
        first = part_start(side, part)
        return pltpu.make_async_remote_copy(
            src_ref=src(first), dst_ref=dst(side, first),
            send_sem=ring_send.at[e, side, part], recv_sem=ring_recv.at[e, side, part],
            device_id=ring_device(1 - 2 * side), device_id_type=MESH)

    def halo_dst(e):
        return lambda side, first: halo.at[e, side, pl.ds(first, 4)]

    def kap_copy(side, part):
        return ring_copy(0, lambda first: kap.at[pl.ds(8 + first, 4), pl.ds(48, ROWS), :], halo_dst(0), side, part)

    def f_copy(side, part):
        return ring_copy(1, lambda first: src_own.at[pl.ds(8 + first, 4)],
                         lambda side, first: src_own.at[pl.ds(16 * side + first, 4)], side, part)

    def u_copy(e, side, part):
        return ring_copy(e, lambda first: stage.at[pl.ds(first, 4)], halo_dst(e), side, part)

    PARTS = [(side, part) for part in range(2) for side in range(2)]

    def unpack_side(e, dst, side, part):
        j = part_start(side, part)
        put(dst, 16 * side + j, halo[e, side, pl.ds(j, 4)])

    pack_array(0)
    pl.semaphore_wait(barrier, 7)
    send_own(0)
    pack_array(1)
    send_own(1)
    pack_array(2)
    send_own(2)

    wait_own(0)
    unpack_own(0, lambda v: put(kap, 8, v))
    kap_copy(fast, 0).start()
    for part in range(2):
        kap_copy(slow, part).start()
    wait_own(1)

    def store_u(v):
        stage[...] = v
        put(fld, 8, v)
    unpack_own(1, store_u)
    u_copy(2, fast, 0).start()
    for part in range(2):
        u_copy(2, slow, part).start()
    kap_copy(fast, 1).start()
    wait_own(2)

    def store_f(v):
        src_own[8:16] = v
    unpack_own(2, store_f)
    f_copy(fast, 0).start()
    for part in range(2):
        f_copy(slow, part).start()
    u_copy(2, fast, 1).start()
    f_copy(fast, 1).start()

    loads[3].wait()
    loads[4].wait()
    half_w = [0.5 * w_ref[n] for n in range(26)]

    def coef_plane(p, _):
        for g in range(4):
            rows = pl.ds(8 * g, 8)
            center = kap[p, 48 + 8 * g:56 + 8 * g, :]
            terms = []
            total = None
            for n, (ox, oy, oz) in enumerate(OFFSETS):
                first = 40 * (oz + 1) + 8 + 8 * g + ox
                near = kap[p + oy, first:first + 8, :]
                c = half_w[n] * (center + near)
                terms.append(c)
                total = c if total is None else total + c
            recip = 1.0 / total
            inv[p, rows, :] = recip
            diag[p, rows, :] = jnp.where(jnp.logical_and(p >= 8, p < 16), total, 0.0)
            for n in range(26):
                coef[p, 40 * n + 8 * g:40 * n + 8 * g + 8, :] = terms[n] * recip
        return 0
    def scale_f(p, _):
        src_div[p] = src_own[p] * inv[p]
        return 0

    def coef_range(lo, hi):
        lax.fori_loop(lo, hi, coef_plane, 0)

    def scale_range(lo, hi):
        lax.fori_loop(lo, hi, scale_f, 0)

    sums[...] = jnp.zeros_like(sums)
    coef_range(9, 15)
    scale_range(9, 15)
    for part in range(2):
        kap_copy(fast, part).wait_recv()
        unpack_side(0, kap, fast, part)
    coef_range(1 + 14 * fast, 9 + 14 * fast)

    def slow_setup(part, left):
        lo = left + slow * (20 - 2 * left)
        kap_copy(slow, part).wait_recv()
        unpack_side(0, kap, slow, part)
        coef_range(lo, lo + 4)
        f_copy(slow, part).wait_recv()
        scale_range(lo, lo + 4)

    def strip(level, left, n, right, before, blk, final=False):
        src = 24 * ((level + 1) % 2)
        dst = 24 - src
        lo = left + right * (24 - n - 2 * left)
        k = DEPTH * blk + level - 1
        turned = fld[pl.ds(before, 4), row(1, 8), :]
        center = fld[pl.ds(src + lo, n), row(1, 8), :]
        acc = src_div[pl.ds(lo, n)] - center
        for ox in (-1, 0, 1):
            for oz in (-1, 0, 1):
                near = fld[pl.ds(src + lo - 1, n + 2), row(oz + 1, 8 + ox), :]
                for oy in (-1, 0, 1):
                    if (ox, oy, oz) != (0, 0, 0):
                        t = 40 * TERM[(ox, oy, oz)]
                        acc = acc + coef[pl.ds(lo, n), t:t + ROWS, :] * near[1 + oy:1 + oy + n]
        new = center + om_ref[k] * acc
        fld[pl.ds(dst + lo, n), row(1, 8), :] = new
        put_turned(fld, before, turned)
        if final:
            stage[pl.ds(lo - 8, n)] = new
        r = acc * diag[pl.ds(lo, n)]
        r = jnp.sum(r * r, axis=0)
        sums[k] = sums[k] + ((r[0:8] + r[8:16]) + (r[16:24] + r[24:32]))
        return dst + lo

    def flush(before):
        put_turned(fld, before, fld[pl.ds(before, 4), row(1, 8), :])
        return before

    def fast_pass(t, before, blk):
        level = 1 + t // 2
        return strip(level, level + 4 * (1 - t % 2), 4, fast, before, blk)

    def block(blk, _):
        e = 2 + blk
        before = strip(1, 9, 3, 0, 8, blk)
        before = flush(strip(1, 9, 3, 1, before, blk))
        before = flush(strip(2, 10, 4, 0, before, blk))
        before = flush(strip(3, 11, 2, 0, before, blk))

        @pl.when(blk == 0)
        def _():
            for part in range(2):
                f_copy(fast, part).wait_recv()
            scale_range(1 + 14 * fast, 9 + 14 * fast)
        for part in range(2):
            u_copy(e, fast, part).wait_recv()
        for part in range(2):
            unpack_side(e, fld, fast, part)
        before = lax.fori_loop(0, 8, lambda t, b: fast_pass(t, b, blk), before)

        @pl.when(blk == 0)
        def _():
            slow_setup(0, 5)
        u_copy(e, slow, 0).wait_recv()
        unpack_side(e, fld, slow, 0)
        before = lax.fori_loop(0, 2, lambda s, b: strip(1 + 4 * s, 5, 4, slow + s * (fast - slow), b, blk), before)
        before = flush(strip(2, 6, 4, slow, before, blk))
        before = strip(3, 7, 4, slow, before, blk)

        @pl.when(blk == 0)
        def _():
            slow_setup(1, 1)
            for side, part in PARTS:
                kap_copy(side, part).wait_send()
                f_copy(side, part).wait_send()
        u_copy(e, slow, 1).wait_recv()
        for side, part in PARTS:
            u_copy(e, side, part).wait_send()
        unpack_side(e, fld, slow, 1)
        before = lax.fori_loop(0, 2, lambda s, b: strip(1 + 3 * s, 1 + 7 * s, 4, slow, b, blk), before)
        before = strip(2, 2, 4, slow, before, blk)
        before = lax.fori_loop(0, 2, lambda s, b: strip(5, 9, 3, s, b, blk), before)
        before = lax.fori_loop(0, 2, lambda s, b: strip(3 + 3 * s, 3 + 7 * s, 4, slow, b, blk), before)
        before = strip(4, 4, 4, slow, before, blk)
        before = strip(7, 11, 2, 0, before, blk)
        before = strip(5, 5, 4, slow, before, blk)
        before = lax.fori_loop(
            0, 4, lambda t, b: strip(6 + t // 2, 6 + t // 2, 4, fast + (t % 2) * (slow - fast), b, blk), before)
        before = lax.fori_loop(0, 2, lambda s, b: strip(8, 8, 4, fast + s * (slow - fast), b, blk, True), before)

        @pl.when(blk < BLOCKS - 1)
        def _():
            for side in (fast, slow):
                for part in range(2):
                    u_copy(e + 1, side, part).start()
            flush(before)
        return 0
    lax.fori_loop(0, BLOCKS, block, 0)

    def sum_copy(r):
        return pltpu.make_async_remote_copy(
            src_ref=psum.at[8], dst_ref=psum.at[me], send_sem=sum_send.at[r - 1], recv_sem=sum_recv.at[r - 1],
            device_id=device((me + r) % 8), device_id_type=MESH)

    def back_copy(r):
        q = (my_q + r) % 4
        return pltpu.make_async_remote_copy(
            src_ref=back.at[q], dst_ref=back_recv.at[my_l], send_sem=back_send.at[r - 1], recv_sem=back_recv_sem.at[r - 1],
            device_id={'batch': 0, 'z': q % 2, 'y': yc, 'x': q // 2}, device_id_type=MESH)

    planes8 = move_lanes(stage[...].reshape(8 * ROWS, LANES), unweave).reshape(8, ROWS, LANES)
    for yy in range(2):
        planes = [planes8[4 * yy + m] for m in range(4)]
        for q in range(4):
            back[q, yy] = jnp.concatenate([v[:, ROWS * q:ROWS * q + ROWS] for v in planes], axis=1)
    for r in range(1, 4):
        back_copy(r).start()
    back_recv[my_l] = back[my_q]
    flat = jnp.sum(sums[...], axis=1)
    flat = jnp.concatenate([flat, jnp.zeros((96, LANES), F32)], axis=0)
    mine = jnp.sum(flat.T, axis=0, keepdims=True)
    mine = jnp.broadcast_to(mine, (8, LANES))
    psum[8] = mine
    psum[me] = mine
    for r in range(1, 8):
        sum_copy(r).start()

    for r in range(1, 4):
        back_copy(r).wait()
    out_ref[...] = back_recv[...]
    for r in range(1, 8):
        sum_copy(r).wait()
    total = psum[0]
    for i in range(1, 8):
        total = total + psum[i]
    rho_ref[...] = total

    for a in range(3):
        for r in range(1, 4):
            own_copy(a, r).wait_send()


def unpack_kernel(dense_ref, total_ref, out_ref, rho_ref):
    for i in range(8):
        v = dense_ref[i // 2, i % 2]
        for m in range(4):
            out_ref[pl.ds(4 * i + m, ROWS, stride=ROWS), :] = v[:, ROWS * m:ROWS * m + ROWS]
    rho_ref[...] = jnp.sqrt(total_ref[...] / CELLS)[0:1, 0:ROWS]


def solution(mesh):
    field_spec = P(('batch', 'x'), 'y', 'z')

    def local(u, f, kappa, w, om):
        vmem = pl.BlockSpec(memory_space=pltpu.VMEM)
        hbm = pl.BlockSpec(memory_space=pltpu.HBM)
        dma = pltpu.SemaphoreType.DMA
        dense, total = pl.pallas_call(
            kernel,
            out_shape=(pltpu.VMEM((4, 2, ROWS, LANES), F32), pltpu.VMEM((8, LANES), F32)),
            in_specs=[hbm] * 5,
            out_specs=(vmem, vmem),
            scratch_shapes=[
                pltpu.SMEM((26,), F32),
                pltpu.SMEM((ROWS,), F32),
                pltpu.VMEM((3 * PITCHED, ROWS), F32),
                dma((5,)),
                pltpu.VMEM((3, 8, ROWS, LANES), F32),
                pltpu.VMEM((3, 4, 2, ROWS, LANES), F32),
                pltpu.VMEM((24, LANES, LANES), F32),
                pltpu.VMEM((48, LANES, LANES), F32),
                pltpu.VMEM((24, 1056, LANES), F32),
                pltpu.VMEM((24, ROWS, LANES), F32),
                pltpu.VMEM((24, ROWS, LANES), F32),
                pltpu.VMEM((24, ROWS, LANES), F32),
                pltpu.VMEM((24, ROWS, LANES), F32),
                pltpu.VMEM((8, ROWS, LANES), F32),
                pltpu.VMEM((6, 2, 8, ROWS, LANES), F32),
                pltpu.VMEM((ROWS, 8, LANES), F32),
                pltpu.VMEM((9, 8, LANES), F32),
                pltpu.VMEM((4, 2, ROWS, LANES), F32),
                pltpu.VMEM((4, 2, ROWS, LANES), F32),
                dma((3, 3)), dma((3, 3)), dma((6, 2, 2)), dma((6, 2, 2)), dma((3,)), dma((3,)), dma((7,)), dma((7,)),
            ],
            compiler_params=pltpu.CompilerParams(collective_id=0, has_side_effects=True, vmem_limit_bytes=60 * MIB),
        )(u, f, kappa, w, om)
        out, rho = pl.pallas_call(
            unpack_kernel,
            out_shape=(jax.ShapeDtypeStruct((ROWS * ROWS, ROWS), F32), jax.ShapeDtypeStruct((1, ROWS), F32)),
            in_specs=[vmem, vmem],
            out_specs=(vmem, vmem),
            compiler_params=pltpu.CompilerParams(vmem_limit_bytes=8 * MIB),
        )(dense, total)
        return out.reshape(ROWS, ROWS, ROWS), rho.reshape(ROWS)

    return jax.shard_map(local, mesh=mesh, in_specs=(field_spec, field_spec, field_spec, P(), P()),
                         out_specs=(field_spec, P('batch')), check_vma=False)
```

```python
import jax
import jax.numpy as jnp
from jax import lax
from jax.experimental import pallas as pl
from jax.experimental.pallas import tpu as pltpu
from jax.sharding import PartitionSpec as P

MESH = pl.DeviceIdType.MESH
F32 = jnp.float32
ROWS = 32
LANES = 128
MIB = 1024 * 1024
PITCH = 40
PITCHED = ROWS * PITCH
DEPTH = 8
BLOCKS = 4
CELLS = 64 * 64 * 64
OFFSETS = [(a, b, c) for a in (-1, 0, 1) for b in (-1, 0, 1) for c in (-1, 0, 1) if (a, b, c) != (0, 0, 0)]
TERM = {o: n for n, o in enumerate(OFFSETS)}


def rows_of(ref):
    return ref.reshape(ROWS, PITCH, ROWS).at[:, pl.ds(0, ROWS), :]


def kernel(u_ref, f_ref, k_ref, w_hbm, om_hbm, out_ref, rho_ref,
           w_ref, om_ref, bricks, brick_sem, pack, recv_own, kap, fld, coef, src_own, src_div, inv, diag, stage, halo, sums, psum, back, back_recv,
           own_send, own_recv, ring_send, ring_recv, back_send, back_recv_sem, sum_send, sum_recv):
    xc = lax.axis_index('x')
    yc = lax.axis_index('y')
    zc = lax.axis_index('z')
    me = 4 * zc + 2 * yc + xc
    turn = (yc + zc) % 2
    my_l = xc + 2 * turn
    my_q = 2 * xc + zc

    fast = 1 - xc
    slow = xc

    def slab_device(slab_y, slab_l):
        t = slab_l // 2
        return {'batch': 0, 'z': (slab_y + t) % 2, 'y': slab_y, 'x': slab_l % 2}

    def ring_device(step):
        s = (4 * yc + my_l + step + 8) % 8
        return slab_device(s // 4, s % 4)

    def flip(bit, swap):
        return 1 - bit if swap else bit

    def partner(r):
        return {'batch': 0, 'z': flip(zc, r & 2), 'y': flip(yc, r & 4), 'x': flip(xc, r & 1)}

    even = lax.broadcasted_iota(jnp.int32, (1, 8, LANES), 2) % 2 == 0
    top = lax.broadcasted_iota(jnp.int32, (1, 8, LANES), 1) == 0
    lane_in = lax.broadcasted_iota(jnp.int32, (LANES, LANES), 0)
    lane_out = lax.broadcasted_iota(jnp.int32, (LANES, LANES), 1)
    weave = (lane_out == 2 * (lane_in % 64) + lane_in // 64).astype(F32).astype(jnp.bfloat16)
    unweave = (lane_in == 2 * (lane_out % 64) + lane_out // 64).astype(F32).astype(jnp.bfloat16)

    def move_lanes(v, matrix):
        total = None
        for _ in range(3):
            part = v.astype(jnp.bfloat16)
            v = v - part.astype(F32)
            moved = jnp.dot(part, matrix, preferred_element_type=F32)
            total = moved if total is None else total + moved
        return total

    loads = [pltpu.make_async_copy(ref, rows_of(bricks.at[pl.ds(a * PITCHED, PITCHED)]), brick_sem.at[a]) for a, ref in enumerate((k_ref, u_ref, f_ref))]
    loads.append(pltpu.make_async_copy(w_hbm, w_ref, brick_sem.at[3]))
    loads.append(pltpu.make_async_copy(om_hbm, om_ref, brick_sem.at[4]))
    for load in loads:
        load.start()

    barrier = pltpu.get_barrier_semaphore()
    for r in range(1, 8):
        pl.semaphore_signal(barrier, inc=1, device_id=partner(r), device_id_type=MESH)

    def pack_array(a):
        loads[a].wait()
        for i in range(8):
            rows = [bricks[pl.ds(a * PITCHED + 4 * i + m, ROWS, stride=PITCH), :] for m in range(4)]
            pack[a, i] = jnp.concatenate(rows, axis=1)

    def own_copy(a, r):
        dest = flip(xc, r & 1) + 2 * flip(turn, r & 2)
        return pltpu.make_async_remote_copy(
            src_ref=pack.at[a, pl.ds(2 * dest, 2)], dst_ref=recv_own.at[a, my_q],
            send_sem=own_send.at[a, r - 1], recv_sem=own_recv.at[a, r - 1],
            device_id=partner(r), device_id_type=MESH)

    def send_own(a):
        for r in range(1, 4):
            own_copy(a, r).start()
        recv_own[a, my_q] = pack[a, pl.ds(2 * my_l, 2)]

    def row(ver, first):
        return slice(40 * ver + first, 40 * ver + first + ROWS)

    def put(dst, plane, v):
        dst[pl.ds(plane, v.shape[0]), row(1, 8), :] = v
        put_turned(dst, plane, v)

    def put_turned(dst, plane, v):
        planes = pl.ds(plane, v.shape[0])
        dst[planes, row(0, 8), :] = pltpu.roll(v, 2, 2)
        dst[planes, row(2, 8), :] = pltpu.roll(v, 126, 2)
        edge = jnp.where(top, v[:, 0:8], v[:, 24:ROWS])
        r1, r3, r125, r127 = (pltpu.roll(edge, s, 2) for s in (1, 3, 125, 127))
        for ver, a, b in ((0, r1, r3), (1, r127, r1), (2, r125, r127)):
            swap = jnp.where(even, a, b)
            dst[planes, 40 * ver + 7:40 * ver + 8, :] = swap[:, 7:8]
            dst[planes, 40 * ver + 40:40 * ver + 41, :] = swap[:, 0:1]

    def wait_own(a):
        for r in range(1, 4):
            own_copy(a, r).wait_recv()

    def unpack_own(a, store):
        planes = [jnp.concatenate([recv_own[a, q, yy, :, ROWS * m:ROWS * m + ROWS] for q in range(4)], axis=1)
                  for yy in range(2) for m in range(4)]
        store(move_lanes(jnp.concatenate(planes, axis=0), weave).reshape(8, ROWS, LANES))

    def part_start(side, part):
        return 4 * (1 - part) * (1 - side) + 4 * part * side

    def ring_copy(e, src, dst, side, part):
        first = part_start(side, part)
        return pltpu.make_async_remote_copy(
            src_ref=src(first), dst_ref=dst(side, first),
            send_sem=ring_send.at[e, side, part], recv_sem=ring_recv.at[e, side, part],
            device_id=ring_device(1 - 2 * side), device_id_type=MESH)

    def halo_dst(e):
        return lambda side, first: halo.at[e, side, pl.ds(first, 4)]

    def kap_copy(side, part):
        return ring_copy(0, lambda first: kap.at[pl.ds(8 + first, 4), pl.ds(48, ROWS), :], halo_dst(0), side, part)

    def f_copy(side, part):
        return ring_copy(1, lambda first: src_own.at[pl.ds(8 + first, 4)],
                         lambda side, first: src_own.at[pl.ds(16 * side + first, 4)], side, part)

    def u_copy(e, side, part):
        return ring_copy(e, lambda first: stage.at[pl.ds(first, 4), pl.ds(0, ROWS), :], halo_dst(e), side, part)

    PARTS = [(side, part) for part in range(2) for side in range(2)]

    def unpack_side(e, dst, side, part):
        j = part_start(side, part)
        put(dst, 16 * side + j, halo[e, side, pl.ds(j, 4)])

    pack_array(0)
    pl.semaphore_wait(barrier, 7)
    send_own(0)
    pack_array(1)
    send_own(1)
    pack_array(2)
    send_own(2)

    wait_own(0)
    unpack_own(0, lambda v: put(kap, 8, v))
    kap_copy(fast, 0).start()
    for part in range(2):
        kap_copy(slow, part).start()
    wait_own(1)

    def store_u(v):
        stage[:, 0:ROWS, :] = v
        put(fld, 8, v)
    unpack_own(1, store_u)
    u_copy(2, fast, 0).start()
    for part in range(2):
        u_copy(2, slow, part).start()
    kap_copy(fast, 1).start()
    wait_own(2)

    def store_f(v):
        src_own[8:16] = v
    unpack_own(2, store_f)
    f_copy(fast, 0).start()
    for part in range(2):
        f_copy(slow, part).start()
    u_copy(2, fast, 1).start()
    f_copy(fast, 1).start()

    loads[3].wait()
    loads[4].wait()
    half_w = [0.5 * w_ref[n] for n in range(26)]

    def coef_plane(p, _):
        for g in range(4):
            rows = pl.ds(8 * g, 8)
            center = kap[p, 48 + 8 * g:56 + 8 * g, :]
            terms = []
            total = None
            for n, (ox, oy, oz) in enumerate(OFFSETS):
                first = 40 * (oz + 1) + 8 + 8 * g + ox
                near = kap[p + oy, first:first + 8, :]
                c = half_w[n] * (center + near)
                terms.append(c)
                total = c if total is None else total + c
            recip = 1.0 / total
            inv[p, rows, :] = recip
            diag[p, rows, :] = jnp.where(jnp.logical_and(p >= 8, p < 16), total, 0.0)
            for n in range(26):
                coef[p, 40 * n + 8 * g:40 * n + 8 * g + 8, :] = terms[n] * recip
        return 0
    def scale_f(p, _):
        src_div[p] = src_own[p] * inv[p]
        return 0

    def coef_range(lo, hi):
        lax.fori_loop(lo, hi, coef_plane, 0)

    def scale_range(lo, hi):
        lax.fori_loop(lo, hi, scale_f, 0)

    sums[...] = jnp.zeros_like(sums)
    coef_range(9, 15)
    scale_range(9, 15)
    for part in range(2):
        kap_copy(fast, part).wait_recv()
        unpack_side(0, kap, fast, part)
    coef_range(1 + 14 * fast, 9 + 14 * fast)

    def slow_setup(part, left):
        lo = left + slow * (20 - 2 * left)
        kap_copy(slow, part).wait_recv()
        unpack_side(0, kap, slow, part)
        coef_range(lo, lo + 4)
        f_copy(slow, part).wait_recv()
        scale_range(lo, lo + 4)

    def strip(level, left, n, right, before, blk, final=False):
        src = 24 * ((level + 1) % 2)
        dst = 24 - src
        lo = left + right * (24 - n - 2 * left)
        k = DEPTH * blk + level - 1
        turned = fld[pl.ds(before, 4), row(1, 8), :]
        acc = src_div[pl.ds(lo, n)]
        for ox in (0, -1, 1):
            for oz in (0, -1, 1):
                near = fld[pl.ds(src + lo - 1, n + 2), row(oz + 1, 8 + ox), :]
                if (ox, oz) == (0, 0):
                    center = near[1:1 + n]
                    acc = acc - center
                for oy in (-1, 0, 1):
                    if (ox, oy, oz) != (0, 0, 0):
                        t = 40 * TERM[(ox, oy, oz)]
                        acc = acc + coef[pl.ds(lo, n), t:t + ROWS, :] * near[1 + oy:1 + oy + n]
        new = center + om_ref[k] * acc
        fld[pl.ds(dst + lo, n), row(1, 8), :] = new
        put_turned(fld, before, turned)
        if final:
            stage[pl.ds(lo - 8, n), 0:ROWS, :] = new
        r = acc * diag[pl.ds(lo, n)]
        r = jnp.sum(r * r, axis=0)
        sums[k] = sums[k] + ((r[0:8] + r[8:16]) + (r[16:24] + r[24:32]))
        return dst + lo

    def flush(before):
        put_turned(fld, before, fld[pl.ds(before, 4), row(1, 8), :])
        return before

    def fast_pass(t, before, blk):
        level = 1 + t // 2
        return strip(level, level + 4 * (1 - t % 2), 4, fast, before, blk)

    def block(blk, _):
        e = 2 + blk
        before = strip(1, 9, 3, 0, 8, blk)
        before = flush(strip(1, 9, 3, 1, before, blk))
        before = flush(strip(2, 10, 4, 0, before, blk))
        before = flush(strip(3, 11, 2, 0, before, blk))

        @pl.when(blk == 0)
        def _():
            for part in range(2):
                f_copy(fast, part).wait_recv()
            scale_range(1 + 14 * fast, 9 + 14 * fast)
        for part in range(2):
            u_copy(e, fast, part).wait_recv()
        for part in range(2):
            unpack_side(e, fld, fast, part)
        before = lax.fori_loop(0, 8, lambda t, b: fast_pass(t, b, blk), before)

        @pl.when(blk == 0)
        def _():
            slow_setup(0, 5)
        u_copy(e, slow, 0).wait_recv()
        unpack_side(e, fld, slow, 0)
        before = lax.fori_loop(0, 2, lambda s, b: strip(1 + 4 * s, 5, 4, slow + s * (fast - slow), b, blk), before)
        before = flush(strip(2, 6, 4, slow, before, blk))
        before = strip(3, 7, 4, slow, before, blk)

        @pl.when(blk == 0)
        def _():
            slow_setup(1, 1)
            for side, part in PARTS:
                kap_copy(side, part).wait_send()
                f_copy(side, part).wait_send()
        u_copy(e, slow, 1).wait_recv()
        for side, part in PARTS:
            u_copy(e, side, part).wait_send()
        unpack_side(e, fld, slow, 1)
        before = lax.fori_loop(0, 2, lambda s, b: strip(1 + 3 * s, 1 + 7 * s, 4, slow, b, blk), before)
        before = strip(2, 2, 4, slow, before, blk)
        before = lax.fori_loop(0, 2, lambda s, b: strip(5, 9, 3, s, b, blk), before)
        before = lax.fori_loop(0, 2, lambda s, b: strip(3 + 3 * s, 3 + 7 * s, 4, slow, b, blk), before)
        before = strip(4, 4, 4, slow, before, blk)
        before = strip(7, 11, 2, 0, before, blk)
        before = strip(5, 5, 4, slow, before, blk)
        before = lax.fori_loop(
            0, 4, lambda t, b: strip(6 + t // 2, 6 + t // 2, 4, fast + (t % 2) * (slow - fast), b, blk), before)
        before = lax.fori_loop(0, 2, lambda s, b: strip(8, 8, 4, fast + s * (slow - fast), b, blk, True), before)

        @pl.when(blk < BLOCKS - 1)
        def _():
            for side in (fast, slow):
                for part in range(2):
                    u_copy(e + 1, side, part).start()
            flush(before)
        return 0
    lax.fori_loop(0, BLOCKS, block, 0)

    def sum_copy(r):
        return pltpu.make_async_remote_copy(
            src_ref=psum.at[8], dst_ref=psum.at[me], send_sem=sum_send.at[r - 1], recv_sem=sum_recv.at[r - 1],
            device_id=partner(r), device_id_type=MESH)

    def back_copy(r, yy):
        q = 2 * flip(xc, r & 1) + flip(zc, r & 2)
        return pltpu.make_async_remote_copy(
            src_ref=back.at[q, yy], dst_ref=back_recv.at[my_l, yy],
            send_sem=back_send.at[yy, r - 1], recv_sem=back_recv_sem.at[yy, r - 1],
            device_id=partner(r), device_id_type=MESH)

    flat_stage = stage.reshape(8 * PITCH, LANES)
    for yy in range(2):
        tiles = [flat_stage[pl.ds(16 * yy + x, 8, stride=PITCH), :] for x in range(16)]
        tiles = move_lanes(jnp.concatenate(tiles, axis=0), unweave).reshape(4, 4, 8, LANES)
        for q in range(4):
            quarter = [tiles[:, m, :, ROWS * q:ROWS * q + ROWS] for m in range(4)]
            back[q, yy] = jnp.concatenate(quarter, axis=2).reshape(ROWS, LANES)
        for r in range(1, 4):
            back_copy(r, yy).start()
    back_recv[my_l] = back[my_q]
    flat = jnp.sum(sums[...], axis=1)
    flat = jnp.concatenate([flat, jnp.zeros((96, LANES), F32)], axis=0)
    mine = jnp.sum(flat.T, axis=0, keepdims=True)
    mine = jnp.broadcast_to(mine, (8, LANES))
    psum[8] = mine
    psum[me] = mine
    for r in range(1, 8):
        sum_copy(r).start()

    for r in range(1, 4):
        for yy in range(2):
            back_copy(r, yy).wait()
    out_ref[...] = back_recv[...]
    for r in range(1, 8):
        sum_copy(r).wait()
    total = psum[0]
    for i in range(1, 8):
        total = total + psum[i]
    rho_ref[...] = total

    for a in range(3):
        for r in range(1, 4):
            own_copy(a, r).wait_send()


def unpack_kernel(dense_ref, total_ref, out_ref, rho_ref):
    for slab in range(4):
        for x in range(ROWS):
            i, m = x % 16 // 4, ROWS * (x % 4)
            first = ROWS * x + 8 * slab
            out_ref[first:first + 8, :] = dense_ref[slab, x // 16, 8 * i:8 * i + 8, m:m + ROWS]
    rho_ref[...] = jnp.sqrt(total_ref[...] / CELLS)[0:1, 0:ROWS]


def solution(mesh):
    field_spec = P(('batch', 'x'), 'y', 'z')

    def local(u, f, kappa, w, om):
        vmem = pl.BlockSpec(memory_space=pltpu.VMEM)
        hbm = pl.BlockSpec(memory_space=pltpu.HBM)
        dma = pltpu.SemaphoreType.DMA
        dense, total = pl.pallas_call(
            kernel,
            out_shape=(pltpu.VMEM((4, 2, ROWS, LANES), F32), pltpu.VMEM((8, LANES), F32)),
            in_specs=[hbm] * 5,
            out_specs=(vmem, vmem),
            scratch_shapes=[
                pltpu.SMEM((26,), F32),
                pltpu.SMEM((ROWS,), F32),
                pltpu.VMEM((3 * PITCHED, ROWS), F32),
                dma((5,)),
                pltpu.VMEM((3, 8, ROWS, LANES), F32),
                pltpu.VMEM((3, 4, 2, ROWS, LANES), F32),
                pltpu.VMEM((24, LANES, LANES), F32),
                pltpu.VMEM((48, LANES, LANES), F32),
                pltpu.VMEM((24, 1056, LANES), F32),
                pltpu.VMEM((24, ROWS, LANES), F32),
                pltpu.VMEM((24, ROWS, LANES), F32),
                pltpu.VMEM((24, ROWS, LANES), F32),
                pltpu.VMEM((24, ROWS, LANES), F32),
                pltpu.VMEM((8, PITCH, LANES), F32),
                pltpu.VMEM((6, 2, 8, ROWS, LANES), F32),
                pltpu.VMEM((ROWS, 8, LANES), F32),
                pltpu.VMEM((9, 8, LANES), F32),
                pltpu.VMEM((4, 2, ROWS, LANES), F32),
                pltpu.VMEM((4, 2, ROWS, LANES), F32),
                dma((3, 3)), dma((3, 3)), dma((6, 2, 2)), dma((6, 2, 2)), dma((2, 3)), dma((2, 3)), dma((7,)), dma((7,)),
            ],
            compiler_params=pltpu.CompilerParams(collective_id=0, has_side_effects=True, vmem_limit_bytes=60 * MIB),
        )(u, f, kappa, w, om)
        out, rho = pl.pallas_call(
            unpack_kernel,
            out_shape=(jax.ShapeDtypeStruct((ROWS * ROWS, ROWS), F32), jax.ShapeDtypeStruct((1, ROWS), F32)),
            in_specs=[vmem, vmem],
            out_specs=(vmem, vmem),
            compiler_params=pltpu.CompilerParams(vmem_limit_bytes=8 * MIB),
        )(dense, total)
        return out.reshape(ROWS, ROWS, ROWS), rho.reshape(ROWS)

    return jax.shard_map(local, mesh=mesh, in_specs=(field_spec, field_spec, field_spec, P(), P()),
                         out_specs=(field_spec, P('batch')), check_vma=False)
```

```python
import jax
import jax.numpy as jnp
from jax import lax
from jax.experimental import pallas as pl
from jax.experimental.pallas import tpu as pltpu
from jax.sharding import PartitionSpec as P

MESH = pl.DeviceIdType.MESH
F32 = jnp.float32
ROWS = 32
LANES = 128
MIB = 1024 * 1024
PITCH = 40
PITCHED = ROWS * PITCH
DEPTH = 8
BLOCKS = 4
CELLS = 64 * 64 * 64
OFFSETS = [(a, b, c) for a in (-1, 0, 1) for b in (-1, 0, 1) for c in (-1, 0, 1) if (a, b, c) != (0, 0, 0)]
TERM = {o: n for n, o in enumerate(OFFSETS)}


def rows_of(ref):
    return ref.reshape(ROWS, PITCH, ROWS).at[:, pl.ds(0, ROWS), :]


def kernel(u_ref, f_ref, k_ref, w_hbm, om_hbm, out_ref, rho_ref,
           w_ref, om_ref, bricks, brick_sem, pack, recv_own, kap, fld, coef, src_own, src_div, inv, diag, stage, halo, sums, psum, back, back_recv,
           own_send, own_recv, ring_send, ring_recv, back_send, back_recv_sem, sum_send, sum_recv):
    xc = lax.axis_index('x')
    yc = lax.axis_index('y')
    zc = lax.axis_index('z')
    me = 4 * zc + 2 * yc + xc
    turn = (yc + zc) % 2
    my_l = xc + 2 * turn
    my_q = 2 * xc + zc

    fast = 1 - xc
    slow = xc

    def slab_device(slab_y, slab_l):
        t = slab_l // 2
        return {'batch': 0, 'z': (slab_y + t) % 2, 'y': slab_y, 'x': slab_l % 2}

    def ring_device(step):
        s = (4 * yc + my_l + step + 8) % 8
        return slab_device(s // 4, s % 4)

    def flip(bit, swap):
        return 1 - bit if swap else bit

    def partner(r):
        return {'batch': 0, 'z': flip(zc, r & 2), 'y': flip(yc, r & 4), 'x': flip(xc, r & 1)}

    even = lax.broadcasted_iota(jnp.int32, (1, 8, LANES), 2) % 2 == 0
    top = lax.broadcasted_iota(jnp.int32, (1, 8, LANES), 1) == 0
    lane_in = lax.broadcasted_iota(jnp.int32, (LANES, LANES), 0)
    lane_out = lax.broadcasted_iota(jnp.int32, (LANES, LANES), 1)
    weave = (lane_out == 2 * (lane_in % 64) + lane_in // 64).astype(F32).astype(jnp.bfloat16)
    unweave = (lane_in == 2 * (lane_out % 64) + lane_out // 64).astype(F32).astype(jnp.bfloat16)

    def move_lanes(v, matrix):
        total = None
        for _ in range(3):
            part = v.astype(jnp.bfloat16)
            v = v - part.astype(F32)
            moved = jnp.dot(part, matrix, preferred_element_type=F32)
            total = moved if total is None else total + moved
        return total

    loads = [pltpu.make_async_copy(ref, rows_of(bricks.at[pl.ds(a * PITCHED, PITCHED)]), brick_sem.at[a]) for a, ref in enumerate((k_ref, u_ref, f_ref))]
    loads.append(pltpu.make_async_copy(w_hbm, w_ref, brick_sem.at[3]))
    loads.append(pltpu.make_async_copy(om_hbm, om_ref, brick_sem.at[4]))
    for load in loads:
        load.start()

    barrier = pltpu.get_barrier_semaphore()
    for r in range(1, 8):
        pl.semaphore_signal(barrier, inc=1, device_id=partner(r), device_id_type=MESH)

    def pack_array(a):
        loads[a].wait()
        for i in range(8):
            rows = [bricks[pl.ds(a * PITCHED + 4 * i + m, ROWS, stride=PITCH), :] for m in range(4)]
            pack[a, i] = jnp.concatenate(rows, axis=1)

    def own_copy(a, r):
        dest = flip(xc, r & 1) + 2 * flip(turn, r & 2)
        return pltpu.make_async_remote_copy(
            src_ref=pack.at[a, pl.ds(2 * dest, 2)], dst_ref=recv_own.at[a, my_q],
            send_sem=own_send.at[a, r - 1], recv_sem=own_recv.at[a, r - 1],
            device_id=partner(r), device_id_type=MESH)

    def send_own(a):
        for r in range(1, 4):
            own_copy(a, r).start()
        recv_own[a, my_q] = pack[a, pl.ds(2 * my_l, 2)]

    def row(ver, first):
        return slice(40 * ver + first, 40 * ver + first + ROWS)

    def put(dst, plane, v):
        dst[pl.ds(plane, v.shape[0]), row(1, 8), :] = v
        put_turned(dst, plane, v)

    def put_turned(dst, plane, v):
        planes = pl.ds(plane, v.shape[0])
        dst[planes, row(0, 8), :] = pltpu.roll(v, 2, 2)
        dst[planes, row(2, 8), :] = pltpu.roll(v, 126, 2)
        edge = jnp.where(top, v[:, 0:8], v[:, 24:ROWS])
        r1, r3, r125, r127 = (pltpu.roll(edge, s, 2) for s in (1, 3, 125, 127))
        for ver, a, b in ((0, r1, r3), (1, r127, r1), (2, r125, r127)):
            swap = jnp.where(even, a, b)
            dst[planes, 40 * ver + 7:40 * ver + 8, :] = swap[:, 7:8]
            dst[planes, 40 * ver + 40:40 * ver + 41, :] = swap[:, 0:1]

    def wait_own(a):
        for r in range(1, 4):
            own_copy(a, r).wait_recv()

    def unpack_own(a, store):
        planes = [jnp.concatenate([recv_own[a, q, yy, :, ROWS * m:ROWS * m + ROWS] for q in range(4)], axis=1)
                  for yy in range(2) for m in range(4)]
        store(move_lanes(jnp.concatenate(planes, axis=0), weave).reshape(8, ROWS, LANES))

    def part_start(side, part):
        return 4 * (1 - part) * (1 - side) + 4 * part * side

    def ring_copy(e, src, dst, side, part):
        first = part_start(side, part)
        return pltpu.make_async_remote_copy(
            src_ref=src(first), dst_ref=dst(side, first),
            send_sem=ring_send.at[e, side, part], recv_sem=ring_recv.at[e, side, part],
            device_id=ring_device(1 - 2 * side), device_id_type=MESH)

    def halo_dst(e):
        return lambda side, first: halo.at[e, side, pl.ds(first, 4)]

    def kap_copy(side, part):
        return ring_copy(0, lambda first: kap.at[pl.ds(8 + first, 4), pl.ds(48, ROWS), :], halo_dst(0), side, part)

    def f_copy(side, part):
        return ring_copy(1, lambda first: src_own.at[pl.ds(8 + first, 4)],
                         lambda side, first: src_own.at[pl.ds(16 * side + first, 4)], side, part)

    def u_copy(e, side, part):
        return ring_copy(e, lambda first: stage.at[pl.ds(first, 4), pl.ds(0, ROWS), :], halo_dst(e), side, part)

    PARTS = [(side, part) for part in range(2) for side in range(2)]

    def unpack_side(e, dst, side, part):
        j = part_start(side, part)
        put(dst, 16 * side + j, halo[e, side, pl.ds(j, 4)])

    pack_array(0)
    pl.semaphore_wait(barrier, 7)
    send_own(0)
    pack_array(1)
    send_own(1)
    pack_array(2)
    send_own(2)

    loads[3].wait()
    loads[4].wait()
    half_w = [0.5 * w_ref[n] for n in range(26)]

    def coef_plane(p, _):
        for g in range(4):
            rows = pl.ds(8 * g, 8)
            center = kap[p, 48 + 8 * g:56 + 8 * g, :]
            terms = []
            total = None
            for n, (ox, oy, oz) in enumerate(OFFSETS):
                first = 40 * (oz + 1) + 8 + 8 * g + ox
                near = kap[p + oy, first:first + 8, :]
                c = half_w[n] * (center + near)
                terms.append(c)
                total = c if total is None else total + c
            recip = 1.0 / total
            inv[p, rows, :] = recip
            diag[p, rows, :] = jnp.where(jnp.logical_and(p >= 8, p < 16), total, 0.0)
            for n in range(26):
                coef[p, 40 * n + 8 * g:40 * n + 8 * g + 8, :] = terms[n] * recip
        return 0
    def scale_f(p, _):
        src_div[p] = src_own[p] * inv[p]
        return 0

    def coef_range(lo, hi):
        lax.fori_loop(lo, hi, coef_plane, 0)

    def scale_range(lo, hi):
        lax.fori_loop(lo, hi, scale_f, 0)

    wait_own(0)
    unpack_own(0, lambda v: put(kap, 8, v))
    kap_copy(fast, 0).start()
    for part in range(2):
        kap_copy(slow, part).start()
    coef_range(9, 15)
    wait_own(1)

    def store_u(v):
        stage[:, 0:ROWS, :] = v
        put(fld, 8, v)
    unpack_own(1, store_u)
    u_copy(2, fast, 0).start()
    for part in range(2):
        u_copy(2, slow, part).start()
    kap_copy(fast, 1).start()
    for part in range(2):
        kap_copy(fast, part).wait_recv()
        unpack_side(0, kap, fast, part)
    coef_range(1 + 14 * fast, 9 + 14 * fast)
    wait_own(2)

    def store_f(v):
        src_own[8:16] = v
    unpack_own(2, store_f)
    f_copy(fast, 0).start()
    for part in range(2):
        f_copy(slow, part).start()
    u_copy(2, fast, 1).start()
    f_copy(fast, 1).start()

    sums[...] = jnp.zeros_like(sums)
    scale_range(9, 15)

    def slow_setup(part, left):
        lo = left + slow * (20 - 2 * left)
        kap_copy(slow, part).wait_recv()
        unpack_side(0, kap, slow, part)
        coef_range(lo, lo + 4)
        f_copy(slow, part).wait_recv()
        scale_range(lo, lo + 4)

    def strip(level, left, n, right, before, blk, final=False):
        src = 24 * ((level + 1) % 2)
        dst = 24 - src
        lo = left + right * (24 - n - 2 * left)
        k = DEPTH * blk + level - 1
        turned = fld[pl.ds(before, 4), row(1, 8), :]
        acc = src_div[pl.ds(lo, n)]
        for ox in (0, -1, 1):
            for oz in (0, -1, 1):
                near = fld[pl.ds(src + lo - 1, n + 2), row(oz + 1, 8 + ox), :]
                if (ox, oz) == (0, 0):
                    center = near[1:1 + n]
                    acc = acc - center
                for oy in (-1, 0, 1):
                    if (ox, oy, oz) != (0, 0, 0):
                        t = 40 * TERM[(ox, oy, oz)]
                        acc = acc + coef[pl.ds(lo, n), t:t + ROWS, :] * near[1 + oy:1 + oy + n]
        new = center + om_ref[k] * acc
        fld[pl.ds(dst + lo, n), row(1, 8), :] = new
        put_turned(fld, before, turned)
        if final:
            stage[pl.ds(lo - 8, n), 0:ROWS, :] = new
        r = acc * diag[pl.ds(lo, n)]
        r = jnp.sum(r * r, axis=0)
        sums[k] = sums[k] + ((r[0:8] + r[8:16]) + (r[16:24] + r[24:32]))
        return dst + lo

    def flush(before):
        put_turned(fld, before, fld[pl.ds(before, 4), row(1, 8), :])
        return before

    def fast_pass(t, before, blk):
        level = 1 + t // 2
        return strip(level, level + 4 * (1 - t % 2), 4, fast, before, blk)

    def block(blk, _):
        e = 2 + blk
        before = strip(1, 9, 3, 0, 8, blk)
        before = flush(strip(1, 9, 3, 1, before, blk))
        before = flush(strip(2, 10, 4, 0, before, blk))
        before = flush(strip(3, 11, 2, 0, before, blk))

        @pl.when(blk == 0)
        def _():
            for part in range(2):
                f_copy(fast, part).wait_recv()
            scale_range(1 + 14 * fast, 9 + 14 * fast)
        for part in range(2):
            u_copy(e, fast, part).wait_recv()
        for part in range(2):
            unpack_side(e, fld, fast, part)
        before = lax.fori_loop(0, 8, lambda t, b: fast_pass(t, b, blk), before)

        @pl.when(blk == 0)
        def _():
            slow_setup(0, 5)
        u_copy(e, slow, 0).wait_recv()
        unpack_side(e, fld, slow, 0)
        before = lax.fori_loop(0, 2, lambda s, b: strip(1 + 4 * s, 5, 4, slow + s * (fast - slow), b, blk), before)
        before = flush(strip(2, 6, 4, slow, before, blk))
        before = strip(3, 7, 4, slow, before, blk)

        @pl.when(blk == 0)
        def _():
            slow_setup(1, 1)
            for side, part in PARTS:
                kap_copy(side, part).wait_send()
                f_copy(side, part).wait_send()
        u_copy(e, slow, 1).wait_recv()
        for side, part in PARTS:
            u_copy(e, side, part).wait_send()
        unpack_side(e, fld, slow, 1)
        before = lax.fori_loop(0, 2, lambda s, b: strip(1 + 3 * s, 1 + 7 * s, 4, slow, b, blk), before)
        before = strip(2, 2, 4, slow, before, blk)
        before = lax.fori_loop(0, 2, lambda s, b: strip(5, 9, 3, s, b, blk), before)
        before = lax.fori_loop(0, 2, lambda s, b: strip(3 + 3 * s, 3 + 7 * s, 4, slow, b, blk), before)
        before = strip(4, 4, 4, slow, before, blk)
        before = strip(7, 11, 2, 0, before, blk)
        before = strip(5, 5, 4, slow, before, blk)
        before = lax.fori_loop(
            0, 4, lambda t, b: strip(6 + t // 2, 6 + t // 2, 4, fast + (t % 2) * (slow - fast), b, blk), before)
        before = lax.fori_loop(0, 2, lambda s, b: strip(8, 8, 4, fast + s * (slow - fast), b, blk, True), before)

        @pl.when(blk < BLOCKS - 1)
        def _():
            for side in (fast, slow):
                for part in range(2):
                    u_copy(e + 1, side, part).start()
            flush(before)
        return 0
    lax.fori_loop(0, BLOCKS, block, 0)

    def sum_copy(r):
        return pltpu.make_async_remote_copy(
            src_ref=psum.at[8], dst_ref=psum.at[me], send_sem=sum_send.at[r - 1], recv_sem=sum_recv.at[r - 1],
            device_id=partner(r), device_id_type=MESH)

    def back_copy(r, yy):
        q = 2 * flip(xc, r & 1) + flip(zc, r & 2)
        return pltpu.make_async_remote_copy(
            src_ref=back.at[q, yy], dst_ref=back_recv.at[my_l, yy],
            send_sem=back_send.at[yy, r - 1], recv_sem=back_recv_sem.at[yy, r - 1],
            device_id=partner(r), device_id_type=MESH)

    flat_stage = stage.reshape(8 * PITCH, LANES)
    for yy in range(2):
        tiles = [flat_stage[pl.ds(16 * yy + x, 8, stride=PITCH), :] for x in range(16)]
        tiles = move_lanes(jnp.concatenate(tiles, axis=0), unweave).reshape(4, 4, 8, LANES)
        for q in range(4):
            quarter = [tiles[:, m, :, ROWS * q:ROWS * q + ROWS] for m in range(4)]
            back[q, yy] = jnp.concatenate(quarter, axis=2).reshape(ROWS, LANES)
        for r in range(1, 4):
            back_copy(r, yy).start()
    back_recv[my_l] = back[my_q]
    flat = jnp.sum(sums[...], axis=1)
    flat = jnp.concatenate([flat, jnp.zeros((96, LANES), F32)], axis=0)
    mine = jnp.sum(flat.T, axis=0, keepdims=True)
    mine = jnp.broadcast_to(mine, (8, LANES))
    psum[8] = mine
    psum[me] = mine
    for r in range(1, 8):
        sum_copy(r).start()

    for r in range(1, 4):
        for yy in range(2):
            back_copy(r, yy).wait()
    out_ref[...] = back_recv[...]
    for r in range(1, 8):
        sum_copy(r).wait()
    total = psum[0]
    for i in range(1, 8):
        total = total + psum[i]
    rho_ref[...] = total

    for a in range(3):
        for r in range(1, 4):
            own_copy(a, r).wait_send()


def unpack_kernel(dense_ref, total_ref, out_ref, rho_ref):
    for slab in range(4):
        for x in range(ROWS):
            i, m = x % 16 // 4, ROWS * (x % 4)
            first = ROWS * x + 8 * slab
            out_ref[first:first + 8, :] = dense_ref[slab, x // 16, 8 * i:8 * i + 8, m:m + ROWS]
    rho_ref[...] = jnp.sqrt(total_ref[...] / CELLS)[0:1, 0:ROWS]


def solution(mesh):
    field_spec = P(('batch', 'x'), 'y', 'z')

    def local(u, f, kappa, w, om):
        vmem = pl.BlockSpec(memory_space=pltpu.VMEM)
        hbm = pl.BlockSpec(memory_space=pltpu.HBM)
        dma = pltpu.SemaphoreType.DMA
        dense, total = pl.pallas_call(
            kernel,
            out_shape=(pltpu.VMEM((4, 2, ROWS, LANES), F32), pltpu.VMEM((8, LANES), F32)),
            in_specs=[hbm] * 5,
            out_specs=(vmem, vmem),
            scratch_shapes=[
                pltpu.SMEM((26,), F32),
                pltpu.SMEM((ROWS,), F32),
                pltpu.VMEM((3 * PITCHED, ROWS), F32),
                dma((5,)),
                pltpu.VMEM((3, 8, ROWS, LANES), F32),
                pltpu.VMEM((3, 4, 2, ROWS, LANES), F32),
                pltpu.VMEM((24, LANES, LANES), F32),
                pltpu.VMEM((48, LANES, LANES), F32),
                pltpu.VMEM((24, 1056, LANES), F32),
                pltpu.VMEM((24, ROWS, LANES), F32),
                pltpu.VMEM((24, ROWS, LANES), F32),
                pltpu.VMEM((24, ROWS, LANES), F32),
                pltpu.VMEM((24, ROWS, LANES), F32),
                pltpu.VMEM((8, PITCH, LANES), F32),
                pltpu.VMEM((6, 2, 8, ROWS, LANES), F32),
                pltpu.VMEM((ROWS, 8, LANES), F32),
                pltpu.VMEM((9, 8, LANES), F32),
                pltpu.VMEM((4, 2, ROWS, LANES), F32),
                pltpu.VMEM((4, 2, ROWS, LANES), F32),
                dma((3, 3)), dma((3, 3)), dma((6, 2, 2)), dma((6, 2, 2)), dma((2, 3)), dma((2, 3)), dma((7,)), dma((7,)),
            ],
            compiler_params=pltpu.CompilerParams(collective_id=0, has_side_effects=True, vmem_limit_bytes=60 * MIB),
        )(u, f, kappa, w, om)
        out, rho = pl.pallas_call(
            unpack_kernel,
            out_shape=(jax.ShapeDtypeStruct((ROWS * ROWS, ROWS), F32), jax.ShapeDtypeStruct((1, ROWS), F32)),
            in_specs=[vmem, vmem],
            out_specs=(vmem, vmem),
            compiler_params=pltpu.CompilerParams(vmem_limit_bytes=8 * MIB),
        )(dense, total)
        return out.reshape(ROWS, ROWS, ROWS), rho.reshape(ROWS)

    return jax.shard_map(local, mesh=mesh, in_specs=(field_spec, field_spec, field_spec, P(), P()),
                         out_specs=(field_spec, P('batch')), check_vma=False)
```

```python
import jax
import jax.numpy as jnp
from jax import lax
from jax.experimental import pallas as pl
from jax.experimental.pallas import tpu as pltpu
from jax.sharding import PartitionSpec as P

MESH = pl.DeviceIdType.MESH
F32 = jnp.float32
ROWS = 32
LANES = 128
MIB = 1024 * 1024
PITCH = 40
PITCHED = ROWS * PITCH
DEPTH = 8
BLOCKS = 4
CELLS = 64 * 64 * 64
OFFSETS = [(a, b, c) for a in (-1, 0, 1) for b in (-1, 0, 1) for c in (-1, 0, 1) if (a, b, c) != (0, 0, 0)]
TERM = {o: n for n, o in enumerate(OFFSETS)}


def rows_of(ref):
    return ref.reshape(ROWS, PITCH, ROWS).at[:, pl.ds(0, ROWS), :]


def kernel(u_ref, f_ref, k_ref, w_hbm, om_hbm, out_ref, rho_ref,
           w_ref, om_ref, bricks, brick_sem, pack, recv_own, kap, fld, coef, src_own, src_div, inv, diag, stage, halo, sums, psum, back, back_recv,
           own_send, own_recv, ring_send, ring_recv, back_send, back_recv_sem, sum_send, sum_recv):
    xc = lax.axis_index('x')
    yc = lax.axis_index('y')
    zc = lax.axis_index('z')
    me = 4 * zc + 2 * yc + xc
    turn = (yc + zc) % 2
    my_l = xc + 2 * turn
    my_q = 2 * xc + zc

    fast = 1 - xc
    slow = xc

    def slab_device(slab_y, slab_l):
        t = slab_l // 2
        return {'batch': 0, 'z': (slab_y + t) % 2, 'y': slab_y, 'x': slab_l % 2}

    def ring_device(step):
        s = (4 * yc + my_l + step + 8) % 8
        return slab_device(s // 4, s % 4)

    def flip(bit, swap):
        return 1 - bit if swap else bit

    def partner(r):
        return {'batch': 0, 'z': flip(zc, r & 2), 'y': flip(yc, r & 4), 'x': flip(xc, r & 1)}

    even = lax.broadcasted_iota(jnp.int32, (1, 8, LANES), 2) % 2 == 0
    top = lax.broadcasted_iota(jnp.int32, (1, 8, LANES), 1) == 0
    lane_in = lax.broadcasted_iota(jnp.int32, (LANES, LANES), 0)
    lane_out = lax.broadcasted_iota(jnp.int32, (LANES, LANES), 1)
    weave = (lane_out == 2 * (lane_in % 64) + lane_in // 64).astype(F32).astype(jnp.bfloat16)
    unweave = (lane_in == 2 * (lane_out % 64) + lane_out // 64).astype(F32).astype(jnp.bfloat16)

    def move_lanes(v, matrix):
        total = None
        for _ in range(3):
            part = v.astype(jnp.bfloat16)
            v = v - part.astype(F32)
            moved = jnp.dot(part, matrix, preferred_element_type=F32)
            total = moved if total is None else total + moved
        return total

    loads = [pltpu.make_async_copy(ref, rows_of(bricks.at[pl.ds(a * PITCHED, PITCHED)]), brick_sem.at[a]) for a, ref in enumerate((k_ref, u_ref, f_ref))]
    loads.append(pltpu.make_async_copy(w_hbm, w_ref, brick_sem.at[3]))
    loads.append(pltpu.make_async_copy(om_hbm, om_ref, brick_sem.at[4]))
    for load in loads:
        load.start()

    barrier = pltpu.get_barrier_semaphore()
    for r in range(1, 8):
        pl.semaphore_signal(barrier, inc=1, device_id=partner(r), device_id_type=MESH)

    def pack_array(a):
        loads[a].wait()
        for i in range(8):
            rows = [bricks[pl.ds(a * PITCHED + 4 * i + m, ROWS, stride=PITCH), :] for m in range(4)]
            pack[a, i] = jnp.concatenate(rows, axis=1)

    def own_copy(a, r):
        dest = flip(xc, r & 1) + 2 * flip(turn, r & 2)
        return pltpu.make_async_remote_copy(
            src_ref=pack.at[a, pl.ds(2 * dest, 2)], dst_ref=recv_own.at[a, my_q],
            send_sem=own_send.at[a, r - 1], recv_sem=own_recv.at[a, r - 1],
            device_id=partner(r), device_id_type=MESH)

    def send_own(a):
        for r in range(1, 4):
            own_copy(a, r).start()
        recv_own[a, my_q] = pack[a, pl.ds(2 * my_l, 2)]

    def row(ver, first):
        return slice(40 * ver + first, 40 * ver + first + ROWS)

    def put(dst, plane, v):
        dst[pl.ds(plane, v.shape[0]), row(1, 8), :] = v
        put_turned(dst, plane, v)

    def put_turned(dst, plane, v):
        planes = pl.ds(plane, v.shape[0])
        dst[planes, row(0, 8), :] = pltpu.roll(v, 2, 2)
        dst[planes, row(2, 8), :] = pltpu.roll(v, 126, 2)
        edge = jnp.where(top, v[:, 0:8], v[:, 24:ROWS])
        r1, r3, r125, r127 = (pltpu.roll(edge, s, 2) for s in (1, 3, 125, 127))
        for ver, a, b in ((0, r1, r3), (1, r127, r1), (2, r125, r127)):
            swap = jnp.where(even, a, b)
            dst[planes, 40 * ver + 7:40 * ver + 8, :] = swap[:, 7:8]
            dst[planes, 40 * ver + 40:40 * ver + 41, :] = swap[:, 0:1]

    def wait_own(a):
        for r in range(1, 4):
            own_copy(a, r).wait_recv()

    def unpack_own(a, store):
        planes = [jnp.concatenate([recv_own[a, q, yy, :, ROWS * m:ROWS * m + ROWS] for q in range(4)], axis=1)
                  for yy in range(2) for m in range(4)]
        store(move_lanes(jnp.concatenate(planes, axis=0), weave).reshape(8, ROWS, LANES))

    def part_start(side, part):
        return 4 * (1 - part) * (1 - side) + 4 * part * side

    def ring_copy(e, src, dst, side, part):
        first = part_start(side, part)
        return pltpu.make_async_remote_copy(
            src_ref=src(first), dst_ref=dst(side, first),
            send_sem=ring_send.at[e, side, part], recv_sem=ring_recv.at[e, side, part],
            device_id=ring_device(1 - 2 * side), device_id_type=MESH)

    def halo_dst(e):
        return lambda side, first: halo.at[e, side, pl.ds(first, 4)]

    def kap_copy(side, part):
        return ring_copy(0, lambda first: kap.at[pl.ds(8 + first, 4), pl.ds(48, ROWS), :], halo_dst(0), side, part)

    def f_copy(side, part):
        return ring_copy(1, lambda first: src_own.at[pl.ds(8 + first, 4)],
                         lambda side, first: src_own.at[pl.ds(16 * side + first, 4)], side, part)

    def u_copy(e, side, part):
        return ring_copy(e, lambda first: stage.at[pl.ds(first, 4), pl.ds(0, ROWS), :], halo_dst(e), side, part)

    PARTS = [(side, part) for part in range(2) for side in range(2)]

    def unpack_side(e, dst, side, part):
        j = part_start(side, part)
        put(dst, 16 * side + j, halo[e, side, pl.ds(j, 4)])

    pack_array(0)
    pl.semaphore_wait(barrier, 7)
    send_own(0)
    pack_array(1)
    send_own(1)
    pack_array(2)
    send_own(2)

    loads[3].wait()
    loads[4].wait()
    half_w = [0.5 * w_ref[n] for n in range(26)]

    def coef_plane(p, _):
        for g in range(4):
            rows = pl.ds(8 * g, 8)
            center = kap[p, 48 + 8 * g:56 + 8 * g, :]
            terms = []
            total = None
            for n, (ox, oy, oz) in enumerate(OFFSETS):
                first = 40 * (oz + 1) + 8 + 8 * g + ox
                near = kap[p + oy, first:first + 8, :]
                c = half_w[n] * (center + near)
                terms.append(c)
                total = c if total is None else total + c
            recip = 1.0 / total
            inv[p, rows, :] = recip
            diag[p, rows, :] = jnp.where(jnp.logical_and(p >= 8, p < 16), total, 0.0)
            for n in range(26):
                coef[p, 40 * n + 8 * g:40 * n + 8 * g + 8, :] = terms[n] * recip
        return 0
    def scale_f(p, _):
        src_div[p] = src_own[p] * inv[p]
        return 0

    def coef_range(lo, hi):
        lax.fori_loop(lo, hi, coef_plane, 0)

    def scale_range(lo, hi):
        lax.fori_loop(lo, hi, scale_f, 0)

    wait_own(0)
    unpack_own(0, lambda v: put(kap, 8, v))
    kap_copy(fast, 0).start()
    for part in range(2):
        kap_copy(slow, part).start()
    coef_range(9, 15)
    wait_own(1)

    def store_u(v):
        stage[:, 0:ROWS, :] = v
        put(fld, 8, v)
    unpack_own(1, store_u)
    u_copy(2, fast, 0).start()
    for part in range(2):
        u_copy(2, slow, part).start()
    kap_copy(fast, 1).start()
    for part in range(2):
        kap_copy(fast, part).wait_recv()
        unpack_side(0, kap, fast, part)
    coef_range(1 + 14 * fast, 9 + 14 * fast)
    wait_own(2)

    def store_f(v):
        src_own[8:16] = v
    unpack_own(2, store_f)
    f_copy(fast, 0).start()
    for part in range(2):
        f_copy(slow, part).start()
    u_copy(2, fast, 1).start()
    f_copy(fast, 1).start()

    sums[...] = jnp.zeros_like(sums)
    scale_range(9, 15)

    def slow_setup(part, left):
        lo = left + slow * (20 - 2 * left)
        kap_copy(slow, part).wait_recv()
        unpack_side(0, kap, slow, part)
        coef_range(lo, lo + 4)
        f_copy(slow, part).wait_recv()
        scale_range(lo, lo + 4)

    def strip(level, left, n, right, before, blk, final=False):
        src = 24 * ((level + 1) % 2)
        dst = 24 - src
        lo = left + right * (24 - n - 2 * left)
        k = DEPTH * blk + level - 1
        turned = fld[pl.ds(before, 4), row(1, 8), :]
        acc = src_div[pl.ds(lo, n)]
        for ox in (0, -1, 1):
            for oz in (0, -1, 1):
                near = fld[pl.ds(src + lo - 1, n + 2), row(oz + 1, 8 + ox), :]
                if (ox, oz) == (0, 0):
                    center = near[1:1 + n]
                    acc = acc - center
                for oy in (-1, 0, 1):
                    if (ox, oy, oz) != (0, 0, 0):
                        t = 40 * TERM[(ox, oy, oz)]
                        acc = acc + coef[pl.ds(lo, n), t:t + ROWS, :] * near[1 + oy:1 + oy + n]
        new = center + om_ref[k] * acc
        fld[pl.ds(dst + lo, n), row(1, 8), :] = new
        put_turned(fld, before, turned)
        if final:
            stage[pl.ds(lo - 8, n), 0:ROWS, :] = new
        r = acc * diag[pl.ds(lo, n)]
        r = jnp.sum(r * r, axis=0)
        sums[k] = sums[k] + ((r[0:8] + r[8:16]) + (r[16:24] + r[24:32]))
        return dst + lo

    def flush(before):
        put_turned(fld, before, fld[pl.ds(before, 4), row(1, 8), :])
        return before

    def fast_pass(t, before, blk):
        level = 1 + t // 2
        return strip(level, level + 4 * (1 - t % 2), 4, fast, before, blk)

    def block(blk, _):
        e = 2 + blk
        before = strip(1, 9, 3, 0, 8, blk)
        before = flush(strip(1, 9, 3, 1, before, blk))
        before = flush(strip(2, 10, 4, 0, before, blk))
        before = strip(3, 11, 2, 0, before, blk)

        @pl.when(blk == 0)
        def _():
            for part in range(2):
                f_copy(fast, part).wait_recv()
            scale_range(1 + 14 * fast, 9 + 14 * fast)
        for part in range(2):
            u_copy(e, fast, part).wait_recv()
        for part in range(2):
            unpack_side(e, fld, fast, part)
        before = lax.fori_loop(0, 8, lambda t, b: fast_pass(t, b, blk), before)

        @pl.when(blk == 0)
        def _():
            slow_setup(0, 5)
        u_copy(e, slow, 0).wait_recv()
        unpack_side(e, fld, slow, 0)
        before = lax.fori_loop(0, 2, lambda s, b: strip(1 + 4 * s, 5, 4, slow + s * (fast - slow), b, blk), before)
        before = flush(strip(2, 6, 4, slow, before, blk))
        before = strip(3, 7, 4, slow, before, blk)

        @pl.when(blk == 0)
        def _():
            slow_setup(1, 1)
            for side, part in PARTS:
                kap_copy(side, part).wait_send()
                f_copy(side, part).wait_send()
        u_copy(e, slow, 1).wait_recv()
        for side, part in PARTS:
            u_copy(e, side, part).wait_send()
        unpack_side(e, fld, slow, 1)
        before = lax.fori_loop(0, 2, lambda s, b: strip(1 + 3 * s, 1 + 7 * s, 4, slow, b, blk), before)
        before = strip(2, 2, 4, slow, before, blk)
        before = lax.fori_loop(0, 2, lambda s, b: strip(5, 9, 3, s, b, blk), before)
        before = lax.fori_loop(0, 2, lambda s, b: strip(3 + 3 * s, 3 + 7 * s, 4, slow, b, blk), before)
        before = strip(4, 4, 4, slow, before, blk)
        before = strip(7, 11, 2, 0, before, blk)
        before = strip(5, 5, 4, slow, before, blk)
        before = lax.fori_loop(
            0, 4, lambda t, b: strip(6 + t // 2, 6 + t // 2, 4, fast + (t % 2) * (slow - fast), b, blk), before)
        before = lax.fori_loop(0, 2, lambda s, b: strip(8, 8, 4, fast + s * (slow - fast), b, blk, True), before)

        @pl.when(blk < BLOCKS - 1)
        def _():
            for side in (fast, slow):
                for part in range(2):
                    u_copy(e + 1, side, part).start()
            flush(before)
        return 0
    lax.fori_loop(0, BLOCKS, block, 0)

    def sum_copy(r):
        return pltpu.make_async_remote_copy(
            src_ref=psum.at[8], dst_ref=psum.at[me], send_sem=sum_send.at[r - 1], recv_sem=sum_recv.at[r - 1],
            device_id=partner(r), device_id_type=MESH)

    def back_copy(r, yy):
        q = 2 * flip(xc, r & 1) + flip(zc, r & 2)
        return pltpu.make_async_remote_copy(
            src_ref=back.at[q, yy], dst_ref=back_recv.at[my_l, yy],
            send_sem=back_send.at[yy, r - 1], recv_sem=back_recv_sem.at[yy, r - 1],
            device_id=partner(r), device_id_type=MESH)

    flat_stage = stage.reshape(8 * PITCH, LANES)
    for yy in range(2):
        tiles = [flat_stage[pl.ds(16 * yy + x, 8, stride=PITCH), :] for x in range(16)]
        tiles = move_lanes(jnp.concatenate(tiles, axis=0), unweave).reshape(4, 4, 8, LANES)
        for q in range(4):
            quarter = [tiles[:, m, :, ROWS * q:ROWS * q + ROWS] for m in range(4)]
            back[q, yy] = jnp.concatenate(quarter, axis=2).reshape(ROWS, LANES)
        for r in range(1, 4):
            back_copy(r, yy).start()
    back_recv[my_l] = back[my_q]
    flat = jnp.sum(sums[...], axis=1)
    flat = jnp.concatenate([flat, jnp.zeros((96, LANES), F32)], axis=0)
    mine = jnp.sum(flat.T, axis=0, keepdims=True)
    mine = jnp.broadcast_to(mine, (8, LANES))
    psum[8] = mine
    psum[me] = mine
    for r in range(1, 8):
        sum_copy(r).start()

    for r in range(1, 4):
        for yy in range(2):
            back_copy(r, yy).wait()
    out_ref[...] = back_recv[...]
    for r in range(1, 8):
        sum_copy(r).wait()
    total = psum[0]
    for i in range(1, 8):
        total = total + psum[i]
    rho_ref[...] = total

    for a in range(3):
        for r in range(1, 4):
            own_copy(a, r).wait_send()


def unpack_kernel(dense_ref, total_ref, out_ref, rho_ref):
    for slab in range(4):
        for x in range(ROWS):
            i, m = x % 16 // 4, ROWS * (x % 4)
            first = ROWS * x + 8 * slab
            out_ref[first:first + 8, :] = dense_ref[slab, x // 16, 8 * i:8 * i + 8, m:m + ROWS]
    rho_ref[...] = jnp.sqrt(total_ref[...] / CELLS)[0:1, 0:ROWS]


def solution(mesh):
    field_spec = P(('batch', 'x'), 'y', 'z')

    def local(u, f, kappa, w, om):
        vmem = pl.BlockSpec(memory_space=pltpu.VMEM)
        hbm = pl.BlockSpec(memory_space=pltpu.HBM)
        dma = pltpu.SemaphoreType.DMA
        dense, total = pl.pallas_call(
            kernel,
            out_shape=(pltpu.VMEM((4, 2, ROWS, LANES), F32), pltpu.VMEM((8, LANES), F32)),
            in_specs=[hbm] * 5,
            out_specs=(vmem, vmem),
            scratch_shapes=[
                pltpu.SMEM((26,), F32),
                pltpu.SMEM((ROWS,), F32),
                pltpu.VMEM((3 * PITCHED, ROWS), F32),
                dma((5,)),
                pltpu.VMEM((3, 8, ROWS, LANES), F32),
                pltpu.VMEM((3, 4, 2, ROWS, LANES), F32),
                pltpu.VMEM((24, LANES, LANES), F32),
                pltpu.VMEM((48, LANES, LANES), F32),
                pltpu.VMEM((24, 1056, LANES), F32),
                pltpu.VMEM((24, ROWS, LANES), F32),
                pltpu.VMEM((24, ROWS, LANES), F32),
                pltpu.VMEM((24, ROWS, LANES), F32),
                pltpu.VMEM((24, ROWS, LANES), F32),
                pltpu.VMEM((8, PITCH, LANES), F32),
                pltpu.VMEM((6, 2, 8, ROWS, LANES), F32),
                pltpu.VMEM((ROWS, 8, LANES), F32),
                pltpu.VMEM((9, 8, LANES), F32),
                pltpu.VMEM((4, 2, ROWS, LANES), F32),
                pltpu.VMEM((4, 2, ROWS, LANES), F32),
                dma((3, 3)), dma((3, 3)), dma((6, 2, 2)), dma((6, 2, 2)), dma((2, 3)), dma((2, 3)), dma((7,)), dma((7,)),
            ],
            compiler_params=pltpu.CompilerParams(collective_id=0, has_side_effects=True, vmem_limit_bytes=60 * MIB),
        )(u, f, kappa, w, om)
        out, rho = pl.pallas_call(
            unpack_kernel,
            out_shape=(jax.ShapeDtypeStruct((ROWS * ROWS, ROWS), F32), jax.ShapeDtypeStruct((1, ROWS), F32)),
            in_specs=[vmem, vmem],
            out_specs=(vmem, vmem),
            compiler_params=pltpu.CompilerParams(vmem_limit_bytes=8 * MIB),
        )(dense, total)
        return out.reshape(ROWS, ROWS, ROWS), rho.reshape(ROWS)

    return jax.shard_map(local, mesh=mesh, in_specs=(field_spec, field_spec, field_spec, P(), P()),
                         out_specs=(field_spec, P('batch')), check_vma=False)
```

```python
import jax
import jax.numpy as jnp
from jax import lax
from jax.experimental import pallas as pl
from jax.experimental.pallas import tpu as pltpu
from jax.sharding import PartitionSpec as P

MESH = pl.DeviceIdType.MESH
F32 = jnp.float32
ROWS = 32
LANES = 128
MIB = 1024 * 1024
PITCH = 40
PITCHED = ROWS * PITCH
DEPTH = 8
BLOCKS = 4
CELLS = 64 * 64 * 64
OFFSETS = [(a, b, c) for a in (-1, 0, 1) for b in (-1, 0, 1) for c in (-1, 0, 1) if (a, b, c) != (0, 0, 0)]
TERM = {o: n for n, o in enumerate(OFFSETS)}


def rows_of(ref):
    return ref.reshape(ROWS, PITCH, ROWS).at[:, pl.ds(0, ROWS), :]


def kernel(u_ref, f_ref, k_ref, w_hbm, om_hbm, out_ref, rho_ref,
           w_ref, om_ref, bricks, brick_sem, pack, recv_own, kap, fld, coef, src_own, src_div, inv, diag, stage, halo, sums, psum, back, back_recv,
           own_send, own_recv, ring_send, ring_recv, back_send, back_recv_sem, sum_send, sum_recv):
    xc = lax.axis_index('x')
    yc = lax.axis_index('y')
    zc = lax.axis_index('z')
    me = 4 * zc + 2 * yc + xc
    turn = (yc + zc) % 2
    my_l = xc + 2 * turn
    my_q = 2 * xc + zc

    fast = 1 - xc
    slow = xc

    def slab_device(slab_y, slab_l):
        t = slab_l // 2
        return {'batch': 0, 'z': (slab_y + t) % 2, 'y': slab_y, 'x': slab_l % 2}

    def ring_device(step):
        s = (4 * yc + my_l + step + 8) % 8
        return slab_device(s // 4, s % 4)

    def flip(bit, swap):
        return 1 - bit if swap else bit

    def partner(r):
        return {'batch': 0, 'z': flip(zc, r & 2), 'y': flip(yc, r & 4), 'x': flip(xc, r & 1)}

    even = lax.broadcasted_iota(jnp.int32, (1, 8, LANES), 2) % 2 == 0
    top = lax.broadcasted_iota(jnp.int32, (1, 8, LANES), 1) == 0
    lane_in = lax.broadcasted_iota(jnp.int32, (LANES, LANES), 0)
    lane_out = lax.broadcasted_iota(jnp.int32, (LANES, LANES), 1)
    weave = (lane_out == 2 * (lane_in % 64) + lane_in // 64).astype(F32).astype(jnp.bfloat16)
    unweave = (lane_in == 2 * (lane_out % 64) + lane_out // 64).astype(F32).astype(jnp.bfloat16)

    def move_lanes(v, matrix):
        total = None
        for _ in range(3):
            part = v.astype(jnp.bfloat16)
            v = v - part.astype(F32)
            moved = jnp.dot(part, matrix, preferred_element_type=F32)
            total = moved if total is None else total + moved
        return total

    loads = [pltpu.make_async_copy(ref, rows_of(bricks.at[pl.ds(a * PITCHED, PITCHED)]), brick_sem.at[a]) for a, ref in enumerate((k_ref, u_ref, f_ref))]
    loads.append(pltpu.make_async_copy(w_hbm, w_ref, brick_sem.at[3]))
    loads.append(pltpu.make_async_copy(om_hbm, om_ref, brick_sem.at[4]))
    for load in loads:
        load.start()

    barrier = pltpu.get_barrier_semaphore()
    for r in range(1, 8):
        pl.semaphore_signal(barrier, inc=1, device_id=partner(r), device_id_type=MESH)

    def pack_array(a):
        loads[a].wait()
        for i in range(8):
            rows = [bricks[pl.ds(a * PITCHED + 4 * i + m, ROWS, stride=PITCH), :] for m in range(4)]
            pack[a, i] = jnp.concatenate(rows, axis=1)

    def own_copy(a, r):
        dest = flip(xc, r & 1) + 2 * flip(turn, r & 2)
        return pltpu.make_async_remote_copy(
            src_ref=pack.at[a, pl.ds(2 * dest, 2)], dst_ref=recv_own.at[a, my_q],
            send_sem=own_send.at[a, r - 1], recv_sem=own_recv.at[a, r - 1],
            device_id=partner(r), device_id_type=MESH)

    def send_own(a):
        for r in range(1, 4):
            own_copy(a, r).start()
        recv_own[a, my_q] = pack[a, pl.ds(2 * my_l, 2)]

    def row(ver, first):
        return slice(40 * ver + first, 40 * ver + first + ROWS)

    def put(dst, plane, v):
        dst[pl.ds(plane, v.shape[0]), row(1, 8), :] = v
        put_turned(dst, plane, v)

    def put_turned(dst, plane, v):
        planes = pl.ds(plane, v.shape[0])
        dst[planes, row(0, 8), :] = pltpu.roll(v, 2, 2)
        dst[planes, row(2, 8), :] = pltpu.roll(v, 126, 2)
        edge = jnp.where(top, v[:, 0:8], v[:, 24:ROWS])
        r1, r3, r125, r127 = (pltpu.roll(edge, s, 2) for s in (1, 3, 125, 127))
        for ver, a, b in ((0, r1, r3), (1, r127, r1), (2, r125, r127)):
            swap = jnp.where(even, a, b)
            dst[planes, 40 * ver + 7:40 * ver + 8, :] = swap[:, 7:8]
            dst[planes, 40 * ver + 40:40 * ver + 41, :] = swap[:, 0:1]

    def wait_own(a):
        for r in range(1, 4):
            own_copy(a, r).wait_recv()

    def unpack_own(a, store):
        planes = [jnp.concatenate([recv_own[a, q, yy, :, ROWS * m:ROWS * m + ROWS] for q in range(4)], axis=1)
                  for yy in range(2) for m in range(4)]
        store(move_lanes(jnp.concatenate(planes, axis=0), weave).reshape(8, ROWS, LANES))

    def part_start(side, part):
        return 4 * (1 - part) * (1 - side) + 4 * part * side

    def ring_copy(e, src, dst, side, part):
        first = part_start(side, part)
        return pltpu.make_async_remote_copy(
            src_ref=src(first), dst_ref=dst(side, first),
            send_sem=ring_send.at[e, side, part], recv_sem=ring_recv.at[e, side, part],
            device_id=ring_device(1 - 2 * side), device_id_type=MESH)

    def halo_dst(e):
        return lambda side, first: halo.at[e, side, pl.ds(first, 4)]

    def kap_copy(side, part):
        return ring_copy(0, lambda first: kap.at[pl.ds(8 + first, 4), pl.ds(48, ROWS), :], halo_dst(0), side, part)

    def f_copy(side, part):
        return ring_copy(1, lambda first: src_own.at[pl.ds(8 + first, 4)],
                         lambda side, first: src_own.at[pl.ds(16 * side + first, 4)], side, part)

    def u_copy(e, side, part):
        return ring_copy(e, lambda first: stage.at[pl.ds(first, 4), pl.ds(0, ROWS), :], halo_dst(e), side, part)

    PARTS = [(side, part) for part in range(2) for side in range(2)]

    def unpack_side(e, dst, side, part):
        j = part_start(side, part)
        put(dst, 16 * side + j, halo[e, side, pl.ds(j, 4)])

    pack_array(0)
    pl.semaphore_wait(barrier, 7)
    send_own(0)
    pack_array(1)
    send_own(1)
    pack_array(2)
    send_own(2)

    loads[3].wait()
    loads[4].wait()
    half_w = [0.5 * w_ref[n] for n in range(26)]

    def coef_plane(p, _):
        for g in range(4):
            rows = pl.ds(8 * g, 8)
            center = kap[p, 48 + 8 * g:56 + 8 * g, :]
            terms = []
            total = None
            for n, (ox, oy, oz) in enumerate(OFFSETS):
                first = 40 * (oz + 1) + 8 + 8 * g + ox
                near = kap[p + oy, first:first + 8, :]
                c = half_w[n] * (center + near)
                terms.append(c)
                total = c if total is None else total + c
            recip = 1.0 / total
            inv[p, rows, :] = recip
            diag[p, rows, :] = jnp.where(jnp.logical_and(p >= 8, p < 16), total, 0.0)
            for n in range(26):
                coef[p, 40 * n + 8 * g:40 * n + 8 * g + 8, :] = terms[n] * recip
        return 0
    def scale_f(p, _):
        src_div[p] = src_own[p] * inv[p]
        return 0

    def coef_range(lo, hi):
        lax.fori_loop(lo, hi, coef_plane, 0)

    def scale_range(lo, hi):
        lax.fori_loop(lo, hi, scale_f, 0)

    wait_own(0)
    unpack_own(0, lambda v: put(kap, 8, v))
    kap_copy(fast, 0).start()
    for part in range(2):
        kap_copy(slow, part).start()
    coef_range(9, 15)
    wait_own(1)

    def store_u(v):
        stage[:, 0:ROWS, :] = v
        put(fld, 8, v)
    unpack_own(1, store_u)
    u_copy(2, fast, 0).start()
    for part in range(2):
        u_copy(2, slow, part).start()
    kap_copy(fast, 1).start()
    for part in range(2):
        kap_copy(fast, part).wait_recv()
        unpack_side(0, kap, fast, part)
    coef_range(1 + 14 * fast, 9 + 14 * fast)
    wait_own(2)

    def store_f(v):
        src_own[8:16] = v
    unpack_own(2, store_f)
    f_copy(fast, 0).start()
    for part in range(2):
        f_copy(slow, part).start()
    u_copy(2, fast, 1).start()
    f_copy(fast, 1).start()

    sums[...] = jnp.zeros_like(sums)
    scale_range(9, 15)

    def slow_setup(part, left):
        lo = left + slow * (20 - 2 * left)
        kap_copy(slow, part).wait_recv()
        unpack_side(0, kap, slow, part)
        coef_range(lo, lo + 4)
        f_copy(slow, part).wait_recv()
        scale_range(lo, lo + 4)

    def strip(level, left, n, right, before, blk, final=False):
        src = 24 * ((level + 1) % 2)
        dst = 24 - src
        lo = left + right * (24 - n - 2 * left)
        k = DEPTH * blk + level - 1
        turned = fld[pl.ds(before, 4), row(1, 8), :]
        acc = src_div[pl.ds(lo, n)]
        for ox in (0, -1, 1):
            for oz in (0, -1, 1):
                near = fld[pl.ds(src + lo - 1, n + 2), row(oz + 1, 8 + ox), :]
                if (ox, oz) == (0, 0):
                    center = near[1:1 + n]
                    acc = acc - center
                for oy in (-1, 0, 1):
                    if (ox, oy, oz) != (0, 0, 0):
                        t = 40 * TERM[(ox, oy, oz)]
                        acc = acc + coef[pl.ds(lo, n), t:t + ROWS, :] * near[1 + oy:1 + oy + n]
        new = center + om_ref[k] * acc
        fld[pl.ds(dst + lo, n), row(1, 8), :] = new
        put_turned(fld, before, turned)
        if final:
            stage[pl.ds(lo - 8, n), 0:ROWS, :] = new
        r = acc * diag[pl.ds(lo, n)]
        r = jnp.sum(r * r, axis=0)
        sums[k] = sums[k] + ((r[0:8] + r[8:16]) + (r[16:24] + r[24:32]))
        return dst + lo

    def flush(before):
        put_turned(fld, before, fld[pl.ds(before, 4), row(1, 8), :])
        return before

    def fast_pass(t, before, blk):
        level = 1 + t // 2
        return strip(level, level + 4 * (1 - t % 2), 4, fast, before, blk)

    def block(blk, _):
        e = 2 + blk
        before = strip(1, 9, 3, 0, 8, blk)
        before = flush(strip(1, 9, 3, 1, before, blk))
        before = flush(strip(2, 10, 4, 0, before, blk))
        before = strip(3, 11, 2, 0, before, blk)

        @pl.when(blk == 0)
        def _():
            for part in range(2):
                f_copy(fast, part).wait_recv()
            scale_range(1 + 14 * fast, 9 + 14 * fast)
        for part in range(2):
            u_copy(e, fast, part).wait_recv()
        for part in range(2):
            unpack_side(e, fld, fast, part)
        before = lax.fori_loop(0, 8, lambda t, b: fast_pass(t, b, blk), before)

        @pl.when(blk == 0)
        def _():
            slow_setup(0, 5)
        u_copy(e, slow, 0).wait_recv()
        unpack_side(e, fld, slow, 0)
        before = lax.fori_loop(0, 2, lambda s, b: strip(1 + 4 * s, 5, 4, slow + s * (fast - slow), b, blk), before)
        before = flush(strip(2, 6, 4, slow, before, blk))
        before = strip(3, 7, 4, slow, before, blk)

        @pl.when(blk == 0)
        def _():
            slow_setup(1, 1)
            for side, part in PARTS:
                kap_copy(side, part).wait_send()
                f_copy(side, part).wait_send()
        u_copy(e, slow, 1).wait_recv()
        for side, part in PARTS:
            u_copy(e, side, part).wait_send()
        unpack_side(e, fld, slow, 1)
        before = lax.fori_loop(0, 2, lambda s, b: strip(1 + 3 * s, 1 + 7 * s, 4, slow, b, blk), before)
        before = strip(2, 2, 4, slow, before, blk)
        before = lax.fori_loop(0, 2, lambda s, b: strip(5, 9, 3, s, b, blk), before)
        before = lax.fori_loop(0, 2, lambda s, b: strip(3 + 3 * s, 3 + 7 * s, 4, slow, b, blk), before)
        before = strip(4, 4, 4, slow, before, blk)
        before = strip(7, 11, 2, 0, before, blk)
        before = strip(5, 5, 4, slow, before, blk)
        before = lax.fori_loop(
            0, 4, lambda t, b: strip(6 + t // 2, 6 + t // 2, 4, fast + (t % 2) * (slow - fast), b, blk), before)
        before = lax.fori_loop(0, 2, lambda s, b: strip(8, 8, 4, fast + s * (slow - fast), b, blk, True), before)

        @pl.when(blk < BLOCKS - 1)
        def _():
            for side in (fast, slow):
                for part in range(2):
                    u_copy(e + 1, side, part).start()
            flush(before)
        return 0
    lax.fori_loop(0, BLOCKS, block, 0)

    def sum_copy(r):
        return pltpu.make_async_remote_copy(
            src_ref=psum.at[8], dst_ref=psum.at[me], send_sem=sum_send.at[r - 1], recv_sem=sum_recv.at[r - 1],
            device_id=partner(r), device_id_type=MESH)

    def back_copy(r, yy):
        q = 2 * flip(xc, r & 1) + flip(zc, r & 2)
        return pltpu.make_async_remote_copy(
            src_ref=back.at[q, yy], dst_ref=back_recv.at[my_l, yy],
            send_sem=back_send.at[yy, r - 1], recv_sem=back_recv_sem.at[yy, r - 1],
            device_id=partner(r), device_id_type=MESH)

    flat = jnp.sum(sums[...], axis=1)
    flat = jnp.concatenate([flat, jnp.zeros((96, LANES), F32)], axis=0)
    mine = jnp.sum(flat.T, axis=0, keepdims=True)
    mine = jnp.broadcast_to(mine, (8, LANES))
    psum[8] = mine
    psum[me] = mine
    for r in range(1, 8):
        sum_copy(r).start()
    flat_stage = stage.reshape(8 * PITCH, LANES)
    for yy in range(2):
        tiles = [flat_stage[pl.ds(16 * yy + x, 8, stride=PITCH), :] for x in range(16)]
        tiles = move_lanes(jnp.concatenate(tiles, axis=0), unweave).reshape(4, 4, 8, LANES)
        for q in range(4):
            quarter = [tiles[:, m, :, ROWS * q:ROWS * q + ROWS] for m in range(4)]
            back[q, yy] = jnp.concatenate(quarter, axis=2).reshape(ROWS, LANES)
        for r in range(1, 4):
            back_copy(r, yy).start()
    back_recv[my_l] = back[my_q]

    for r in range(1, 4):
        for yy in range(2):
            back_copy(r, yy).wait()
    out_ref[...] = back_recv[...]
    for r in range(1, 8):
        sum_copy(r).wait()
    total = psum[0]
    for i in range(1, 8):
        total = total + psum[i]
    rho_ref[...] = total

    for a in range(3):
        for r in range(1, 4):
            own_copy(a, r).wait_send()


def unpack_kernel(dense_ref, total_ref, out_ref, rho_ref):
    for slab in range(4):
        for x in range(ROWS):
            i, m = x % 16 // 4, ROWS * (x % 4)
            first = ROWS * x + 8 * slab
            out_ref[first:first + 8, :] = dense_ref[slab, x // 16, 8 * i:8 * i + 8, m:m + ROWS]
    rho_ref[...] = jnp.sqrt(total_ref[...] / CELLS)[0:1, 0:ROWS]


def solution(mesh):
    field_spec = P(('batch', 'x'), 'y', 'z')

    def local(u, f, kappa, w, om):
        vmem = pl.BlockSpec(memory_space=pltpu.VMEM)
        hbm = pl.BlockSpec(memory_space=pltpu.HBM)
        dma = pltpu.SemaphoreType.DMA
        dense, total = pl.pallas_call(
            kernel,
            out_shape=(pltpu.VMEM((4, 2, ROWS, LANES), F32), pltpu.VMEM((8, LANES), F32)),
            in_specs=[hbm] * 5,
            out_specs=(vmem, vmem),
            scratch_shapes=[
                pltpu.SMEM((26,), F32),
                pltpu.SMEM((ROWS,), F32),
                pltpu.VMEM((3 * PITCHED, ROWS), F32),
                dma((5,)),
                pltpu.VMEM((3, 8, ROWS, LANES), F32),
                pltpu.VMEM((3, 4, 2, ROWS, LANES), F32),
                pltpu.VMEM((24, LANES, LANES), F32),
                pltpu.VMEM((48, LANES, LANES), F32),
                pltpu.VMEM((24, 1056, LANES), F32),
                pltpu.VMEM((24, ROWS, LANES), F32),
                pltpu.VMEM((24, ROWS, LANES), F32),
                pltpu.VMEM((24, ROWS, LANES), F32),
                pltpu.VMEM((24, ROWS, LANES), F32),
                pltpu.VMEM((8, PITCH, LANES), F32),
                pltpu.VMEM((6, 2, 8, ROWS, LANES), F32),
                pltpu.VMEM((ROWS, 8, LANES), F32),
                pltpu.VMEM((9, 8, LANES), F32),
                pltpu.VMEM((4, 2, ROWS, LANES), F32),
                pltpu.VMEM((4, 2, ROWS, LANES), F32),
                dma((3, 3)), dma((3, 3)), dma((6, 2, 2)), dma((6, 2, 2)), dma((2, 3)), dma((2, 3)), dma((7,)), dma((7,)),
            ],
            compiler_params=pltpu.CompilerParams(collective_id=0, has_side_effects=True, vmem_limit_bytes=60 * MIB),
        )(u, f, kappa, w, om)
        out, rho = pl.pallas_call(
            unpack_kernel,
            out_shape=(jax.ShapeDtypeStruct((ROWS * ROWS, ROWS), F32), jax.ShapeDtypeStruct((1, ROWS), F32)),
            in_specs=[vmem, vmem],
            out_specs=(vmem, vmem),
            compiler_params=pltpu.CompilerParams(vmem_limit_bytes=8 * MIB),
        )(dense, total)
        return out.reshape(ROWS, ROWS, ROWS), rho.reshape(ROWS)

    return jax.shard_map(local, mesh=mesh, in_specs=(field_spec, field_spec, field_spec, P(), P()),
                         out_specs=(field_spec, P('batch')), check_vma=False)
```
